512 devices in a mesh: cp: 128 (over z, y, core), tp: 4 (over x).
Axes of the slice: x: 4, y: 8, z: 8, core: 2. Of those that a mesh axis runs over, the one named last changes fastest.
Arguments:
- queries: bfloat16 [49152, 4096], P('cp', 'tp'), may hold values from -56 to 56
- keys: bfloat16 [49152, 1024], P('cp', 'tp'), may hold values from -6 to 6
- values: bfloat16 [49152, 1024], P('cp', 'tp'), may hold values from -6 to 6
- lengths: int32 [32], replicated, may hold values from 1 to 2689, 49152 in all
Outputs:
- attended: bfloat16 [49152, 4096], P('cp', 'tp')
The draws below stay inside these ranges and needn't reach their ends.
Inputs may be any that keep to these rules, and one draw needn't show every extreme that they name: `lengths`: the 32 documents fill the 49152 tokens; each has at most 2689 tokens and one has exactly 2689.
All inputs are finite; a program needn't handle non-finite values.
Results may differ from the reference program's by a relative error of at most 0.0065.
Values may be sent and summed in bfloat16 or wider, within the bound.
A program may use at most 64 MiB of HBM per device.

```python
import math
import jax
import jax.numpy as jnp
import numpy as np
from jax import lax

HEADS = 32
KV_HEADS = 8
HEAD_DIM = 128
TOK_DEV = 384
SPAN = 8
DOC_MOST = 2689
NDOCS = 32
TOKENS = 49152
N_CP = 128


def shared_keys(key):
    base = jnp.clip(jax.random.normal(jax.random.fold_in(key, 11), (TOKENS, KV_HEADS * HEAD_DIM), jnp.float32), -4.5, 4.5)
    return base


def draw_keys(key, part):
    return shared_keys(key).astype(jnp.bfloat16)


def draw_queries(key, part):
    base = jnp.clip(jax.random.normal(jax.random.fold_in(key, 13), (TOKENS, HEADS * HEAD_DIM), jnp.float32), -4.5, 4.5)
    return base.astype(jnp.bfloat16)


def levels(own_key, shape, pieces, least, largest):
    def one(dim, parts):
        draws = jax.random.uniform(jax.random.fold_in(jax.random.fold_in(own_key, 6), dim), (parts,), jnp.float32, least / len(pieces), largest / len(pieces))
        return jnp.repeat(jnp.exp(draws), shape[dim] // parts).reshape((-1,) + (1,) * (len(shape) - dim - 1))

    factor_of = one(*pieces[0])
    for cut in pieces[1:]:
        factor_of = factor_of * one(*cut)
    return factor_of


def split_up(count, total, most, slope):
    loads = [(1 << 20) // math.isqrt(standing ** slope) + 1 for standing in range(2, count + 1)]
    spare, counts = total - most - (count - 1), [1] * (count - 1)
    while spare > 0:
        free = [i for i in range(count - 1) if counts[i] < most]
        whole, left = sum([loads[i] for i in free]), spare
        for i in free:
            addition = min(most - counts[i], max(1, left * loads[i] // whole), spare)
            counts[i] = counts[i] + addition
            spare = spare - addition
    return np.array([most] + counts)


def ragged_sizes(stream_key, amount, total, reach, slope):
    if amount == 2:
        one = jax.random.randint(stream_key, (), max(1, total - reach), min(reach, total - 1) + 1)
        return jnp.stack([one, total - one])
    sizes = jnp.asarray(split_up(amount, total, reach, slope), jnp.int32)
    couples = (amount - 1) // 2
    giver, receiver = sizes[1:1 + 2 * couples:2], sizes[2:2 + 2 * couples:2]
    margin = jnp.minimum(giver - 1, reach - receiver)
    shifted = jax.random.randint(jax.random.fold_in(stream_key, 1), (couples,), 0, 1 << 20) % (margin + 1)
    sizes = sizes.at[1:1 + 2 * couples:2].set(giver - shifted).at[2:2 + 2 * couples:2].set(receiver + shifted)
    return sizes[jax.random.permutation(jax.random.fold_in(stream_key, 2), amount)]


def scatter_about(key, extent, deviation, reach, split=(), kind=jnp.bfloat16):
    drawn = deviation * jax.random.normal(key, extent, jnp.float32)
    if split:
        drawn = drawn * levels(key, extent, split, -0.22, 0.18)
    return jnp.clip(drawn, -reach, reach).astype(kind)


def setup_inputs(seed: int = 0) -> dict:
    key_of = jax.random.split(jax.random.key(seed), 5)
    return {
        "queries": draw_queries(jax.random.fold_in(key_of[4], 71), 0),
        "keys": draw_keys(jax.random.fold_in(key_of[4], 71), 0),
        "values": scatter_about(key_of[2], (TOKENS, KV_HEADS * HEAD_DIM), 1.0, 6.0, ((0, 128), (1, 4))),
        "lengths": ragged_sizes(key_of[3], NDOCS, TOKENS, DOC_MOST, 2).astype(jnp.int32),
    }


def document_of(doc_starts, position):
    return jnp.sum((doc_starts[None, :] <= position[:, None]).astype(jnp.int32), axis=1) - 1


def reference(queries, keys, values, lengths):
    doc_ends = jnp.cumsum(lengths)
    doc_starts = doc_ends - lengths
    group_size = HEADS // KV_HEADS
    padding = (SPAN - 1) * TOK_DEV
    window = SPAN * TOK_DEV
    logit_scale_factor = HEAD_DIM ** -0.5
    key_pad = jnp.concatenate([jnp.zeros((padding, keys.shape[1]), keys.dtype), keys], axis=0)
    value_pad = jnp.concatenate([jnp.zeros((padding, values.shape[1]), values.dtype), values], axis=0)

    def one_block(block_index):
        anchor = (block_index * TOK_DEV).astype(jnp.int32)
        query_matrix_rows = lax.dynamic_slice_in_dim(queries, anchor, TOK_DEV, 0).astype(jnp.float32)
        query_matrix_rows = query_matrix_rows.reshape(TOK_DEV, KV_HEADS, group_size, HEAD_DIM)
        key_matrix_rows = lax.dynamic_slice_in_dim(key_pad, anchor, window, 0).astype(jnp.float32)
        key_matrix_rows = key_matrix_rows.reshape(window, KV_HEADS, HEAD_DIM)
        value_matrix_rows = lax.dynamic_slice_in_dim(value_pad, anchor, window, 0).astype(jnp.float32)
        value_matrix_rows = value_matrix_rows.reshape(window, KV_HEADS, HEAD_DIM)
        query_pos = anchor + jnp.arange(TOK_DEV, dtype=jnp.int32)
        key_pos = anchor - padding + jnp.arange(window, dtype=jnp.int32)
        allowed = (document_of(doc_starts, query_pos)[:, None] == document_of(doc_starts, key_pos)[None, :])
        allowed = allowed & (key_pos[None, :] <= query_pos[:, None]) & (key_pos[None, :] >= 0)
        attention_logits = jnp.einsum("yxau,kxu->xayk", query_matrix_rows, key_matrix_rows) * logit_scale_factor
        attention_logits = jnp.where(allowed, attention_logits, -1e30)
        row_max = jnp.max(attention_logits, axis=-1)
        weights = jnp.where(allowed, jnp.exp(attention_logits - row_max[..., None]), 0.0)
        total = jnp.sum(weights, axis=-1)
        lower_bound = weights.astype(jnp.bfloat16).astype(jnp.float32)
        weighted_value_sum = jnp.einsum("cqla,acf->cqlf", lower_bound, value_matrix_rows)
        result = weighted_value_sum / total[..., None]
        return result.transpose(2, 0, 1, 3).reshape(TOK_DEV, HEADS * HEAD_DIM).astype(jnp.bfloat16)

    blocks = lax.map(one_block, jnp.arange(N_CP, dtype=jnp.int32))
    return blocks.reshape(TOKENS, HEADS * HEAD_DIM)
```

```python
import functools
import math

import jax
import jax.numpy as jnp
from jax import lax
from jax.experimental import pallas as pl
from jax.experimental.pallas import tpu as pltpu
from jax.sharding import PartitionSpec as P

HEAD_DIM = 128
RING_Y = 8
HALVES = ((0, 256), (256, 128))
MASKED = -1e30
FAR = 6
LANDED = 7
RELAY = 8
OWN = 9
SLOTS = 10


def kernel(count, q_hbm, k_hbm, v_hbm, lengths, out_hbm,
           kv, q_in, qt, acc, top, total, first_live, bias, out_v,
           load_sem, out_sem, recv_sem, own_sem, relay_sem, cross_sem):
    toks = q_in.shape[0]
    heads = q_in.shape[1] // HEAD_DIM
    group = heads // (k_hbm.shape[1] // HEAD_DIM)
    factor = HEAD_DIM ** -0.5 * math.log2(math.e)
    cp = lax.axis_index("cp")
    chip, core = cp // 2, lax.rem(cp, 2)
    chips = count // 2
    y = lax.rem(chip, RING_Y)
    row = chip - y

    def core_of(which_chip):
        return lax.rem(which_chip + chips, chips) * 2 + core

    partner = chip * 2 + (1 - core)
    after, before = core_of(chip + 1), core_of(chip - 1)
    three_down = core_of(row + lax.rem(y + RING_Y - 3, RING_Y))
    three_up = core_of(row + lax.rem(y + 3, RING_Y))
    relay_to = core_of(row + lax.rem(y + 3, RING_Y) + 4)
    owner = lax.rem(chip - 4 + chips, chips)
    owner_y = lax.rem(owner, RING_Y)
    relay_from = core_of(owner - owner_y + lax.rem(owner_y + RING_Y - 3, RING_Y))

    def piece(slot, p):
        first, rows = HALVES[p // 2]
        return kv.at[p % 2, slot, pl.ds(first, rows), :]

    def remote(src, dst, send, recv, to):
        return pltpu.make_async_remote_copy(
            src_ref=src, dst_ref=dst, send_sem=send, recv_sem=recv,
            device_id={"cp": to}, device_id_type=pl.DeviceIdType.MESH)

    loads = []
    for source, target, sem in ((k_hbm, kv.at[0, OWN], 0), (v_hbm, kv.at[1, OWN], 1), (q_hbm, q_in, 2)):
        copy = pltpu.make_async_copy(source, target, load_sem.at[sem])
        copy.start()
        loads.append(copy)

    barrier = pltpu.get_barrier_semaphore()

    def greet(devices):
        for device in devices:
            pl.semaphore_signal(barrier, inc=1, device_id={"cp": device}, device_id_type=pl.DeviceIdType.MESH)
        pl.semaphore_wait(barrier, len(devices))

    @pl.when(core == 0)
    def _():
        greet((partner, after, before))

    @pl.when(core == 1)
    def _():
        greet((partner, after, before, three_down, three_up, relay_to, relay_from))

    loads[0].wait()
    loads[1].wait()

    def own_send(lane, p):
        to, slot = ((after, core), (partner, FAR), (three_down, RELAY))[lane]
        return remote(piece(OWN, p), piece(slot, p), own_sem.at[lane, p], recv_sem.at[slot, p], to)

    def relay(slot, p):
        to, target = {0: (after, 2), 1: (after, 3), 2: (after, 4), RELAY: (relay_to, LANDED), LANDED: (before, 5)}[slot]
        return remote(piece(slot, p), piece(target, p), relay_sem.at[slot, p], recv_sem.at[target, p], to)

    def cross(slot, p):
        target = FAR if slot == LANDED else slot
        return remote(piece(slot, p), piece(target, p), cross_sem.at[slot, p], recv_sem.at[target, p], partner)

    def arrived(slot, p):
        remote(piece(slot, p), piece(slot, p), cross_sem.at[slot, p], recv_sem.at[slot, p], partner).wait_recv()

    relayed = {0: (0, 2), 1: (1, RELAY, LANDED)}
    crossed = {0: (0, 2, 4), 1: (1, 3, LANDED, 5)}
    own_lanes = {0: (0, 1), 1: (0, 2)}

    def event(me, slot, pieces):
        for p in pieces:
            arrived(slot, p)
            if slot in relayed[me]:
                relay(slot, p).start()
            if slot in crossed[me]:
                cross(slot, p).start()

    def on(me, *ops):
        @pl.when(core == me)
        def _():
            for op in ops:
                event(me, *op)

    for me in (0, 1):
        @pl.when(core == me)
        def _():
            for p in range(4):
                for lane in own_lanes[me]:
                    own_send(lane, p).start()

    query_pos = cp * toks + lax.broadcasted_iota(jnp.int32, (1, toks), 1)
    starts = jnp.zeros((1, toks), jnp.int32)
    position = jnp.int32(0)
    for doc in range(lengths.shape[0]):
        starts = jnp.where(query_pos >= position, position, starts)
        position = position + lengths[doc]
    first_live[...] = starts

    loads[2].wait()
    for h in range(heads):
        qt[h] = q_in[:, h * HEAD_DIM : (h + 1) * HEAD_DIM].T
    acc[...] = jnp.zeros_like(acc)
    total[...] = jnp.zeros_like(total)
    top[...] = jnp.full_like(top, MASKED)

    def absorb(slot, half, block, diagonal=False):
        first, rows = HALVES[half]
        key_pos = block * toks + first + lax.broadcasted_iota(jnp.int32, (rows, toks), 0)
        live = key_pos >= first_live[...]
        if diagonal:
            live = live & (key_pos <= cp * toks + lax.broadcasted_iota(jnp.int32, (rows, toks), 1))
        bias[:rows] = jnp.where(live, 0.0, MASKED)
        for g in range(heads // group):
            columns = slice(g * HEAD_DIM, (g + 1) * HEAD_DIM)
            keys = kv[0, slot, first : first + rows, columns]
            values = kv[1, slot, first : first + rows, columns].T
            for h in range(g * group, (g + 1) * group):
                scores = jnp.dot(keys, qt[h], preferred_element_type=jnp.float32) + bias[:rows]
                old = top[h : h + 1]
                new = jnp.maximum(old, jnp.max(scores, axis=0, keepdims=True))
                weights = jnp.exp2((scores - new) * factor)
                rescale = jnp.exp2((old - new) * factor)
                top[h : h + 1] = new
                total[h : h + 1] = total[h : h + 1] * rescale + jnp.sum(weights, axis=0, keepdims=True)
                acc[h] = acc[h] * rescale + jnp.dot(
                    values, weights.astype(jnp.bfloat16), preferred_element_type=jnp.float32)

    absorb(OWN, 0, cp, diagonal=True)
    absorb(OWN, 1, cp, diagonal=True)

    H = ((0, 1), (2, 3))
    steps0 = ((0, 0), (1, 0), (0, 1), (1, 1), (2, 0), (3, 0), (2, 1), (3, 1), (FAR, 0), (FAR, 1), (4, 0), (5, 0), (4, 1), (5, 1))
    steps1 = ((FAR, 0), (0, 0), (FAR, 1), (0, 1), (1, 0), (2, 0), (1, 1), (2, 1), (3, 0), (3, 1), (4, 0), (5, 0), (4, 1), (5, 1))
    ahead0 = {t: ((slot, H[half]),) for t, (slot, half) in enumerate(steps0)}
    ahead1 = {
        0: ((FAR, H[0]),),
        1: ((1, H[0]), (RELAY, (0,)), (0, H[0])),
        2: ((FAR, H[1]),),
        3: ((RELAY, (1,)), (1, H[1]), (0, H[1])),
        5: ((RELAY, (2,)), (3, H[0]), (2, H[0])),
        7: ((RELAY, (3,)), (LANDED, (0, 1, 2)), (3, H[1]), (LANDED, (3,)), (2, H[1])),
        10: ((5, H[0]), (4, H[0])),
        12: ((5, H[1]), (4, H[1])),
    }
    for t in range(len(steps0)):
        if t in ahead0:
            on(0, *ahead0[t])
        if t in ahead1:
            on(1, *ahead1[t])
        (slot0, half), (slot1, half1) = steps0[t], steps1[t]
        assert half == half1
        slot = slot0 if slot0 == slot1 else jnp.where(core == 0, slot0, slot1)

        def block_of(slot, me):
            if slot == FAR:
                return 2 * chip - 7 if me == 0 else 2 * chip
            return 2 * (chip - slot // 2 - 1) + slot % 2

        absorb(slot, half, jnp.where(core == 0, block_of(slot0, 0), block_of(slot1, 1)))

    stores = []
    for h in range(heads):
        columns = slice(h * HEAD_DIM, (h + 1) * HEAD_DIM)
        out_v[:, columns] = (acc[h] / total[h : h + 1]).T.astype(out_v.dtype)
        if h % group == group - 1:
            columns = pl.ds((h + 1 - group) * HEAD_DIM, group * HEAD_DIM)
            copy = pltpu.make_async_copy(out_v.at[:, columns], out_hbm.at[:, columns], out_sem.at[h // group])
            copy.start()
            stores.append(copy)
    for me in (0, 1):
        @pl.when(core == me)
        def _():
            for p in range(4):
                for lane in own_lanes[me]:
                    own_send(lane, p).wait_send()
                for slot in relayed[me]:
                    relay(slot, p).wait_send()
                for slot in crossed[me]:
                    cross(slot, p).wait_send()
    for copy in stores:
        copy.wait()


def body(count, queries, keys, values, lengths):
    toks, wide = queries.shape
    heads = wide // HEAD_DIM
    return pl.pallas_call(
        functools.partial(kernel, count),
        out_shape=jax.ShapeDtypeStruct((toks, wide), jnp.bfloat16),
        in_specs=[pl.BlockSpec(memory_space=pl.ANY)] * 3 + [pl.BlockSpec(memory_space=pltpu.SMEM)],
        out_specs=pl.BlockSpec(memory_space=pl.ANY),
        scratch_shapes=[
            pltpu.VMEM((2, SLOTS, toks, keys.shape[1]), jnp.bfloat16),
            pltpu.VMEM((toks, wide), jnp.bfloat16),
            pltpu.VMEM((heads, HEAD_DIM, toks), jnp.bfloat16),
            pltpu.VMEM((heads, HEAD_DIM, toks), jnp.float32),
            pltpu.VMEM((heads, toks), jnp.float32),
            pltpu.VMEM((heads, toks), jnp.float32),
            pltpu.VMEM((1, toks), jnp.int32),
            pltpu.VMEM((HALVES[0][1], toks), jnp.float32),
            pltpu.VMEM((toks, wide), jnp.bfloat16),
            pltpu.SemaphoreType.DMA((3,)),
            pltpu.SemaphoreType.DMA((2,)),
            pltpu.SemaphoreType.DMA((SLOTS, 4)),
            pltpu.SemaphoreType.DMA((3, 4)),
            pltpu.SemaphoreType.DMA((SLOTS, 4)),
            pltpu.SemaphoreType.DMA((SLOTS, 4)),
        ],
        compiler_params=pltpu.CompilerParams(collective_id=0, has_side_effects=True),
    )(queries, keys, values, lengths)


def solution(mesh):
    in_specs = (P("cp", "tp"), P("cp", "tp"), P("cp", "tp"), P())
    return jax.shard_map(functools.partial(body, mesh.shape["cp"]), mesh=mesh, in_specs=in_specs,
                         out_specs=P("cp", "tp"), check_vma=False)
```

```python
import functools
import math

import jax
import jax.numpy as jnp
from jax import lax
from jax.experimental import pallas as pl
from jax.experimental.pallas import tpu as pltpu
from jax.sharding import PartitionSpec as P

HEAD_DIM = 128
RING_Y = 8
PAIR = 2
MASKED = -1e30
FAR = 6
LANDED = 7
RELAY = 8
OWN = 9
SLOTS = 10
FIRST, SECOND = (0, 1), (2, 3)
STEPS = 16
AHEAD = (
    {2: ((0, FIRST),), 3: ((1, FIRST),), 4: ((0, SECOND),), 5: ((1, SECOND),),
     6: ((2, FIRST),), 7: ((3, FIRST),), 8: ((2, SECOND),), 9: ((3, SECOND),),
     10: ((FAR, FIRST),), 11: ((FAR, SECOND),),
     12: ((4, FIRST),), 13: ((5, FIRST),), 14: ((4, SECOND),), 15: ((5, SECOND),)},
    {2: ((FAR, FIRST),), 3: ((FAR, SECOND),),
     4: ((1, FIRST), (RELAY, (0,)), (0, FIRST)), 6: ((RELAY, (1,)), (1, SECOND), (0, SECOND)),
     8: ((RELAY, (2,)), (3, FIRST), (2, FIRST)),
     10: ((RELAY, (3,)), (LANDED, (0, 1, 2)), (3, SECOND), (LANDED, (3,)), (2, SECOND)),
     12: ((5, FIRST), (4, FIRST)), 14: ((5, SECOND), (4, SECOND))},
)
OWN_LANES = ((0, 1), (0, 2))
RELAYED = ((0, 2), (1, RELAY, LANDED))
CROSSED = ((0, 2, 4), (1, 3, LANDED, 5))


def kernel(count, q_hbm, k_hbm, v_hbm, lengths, out_hbm,
           kv, q_in, qt, acc, top, total, first_live, bias, scores, weights, old_top, new_top, rescale, out_v,
           load_sem, out_sem, recv_sem, own_sem, relay_sem, cross_sem):
    toks = q_in.shape[0]
    kv_heads = kv.shape[2]
    heads = q_in.shape[1] // HEAD_DIM
    group = heads // kv_heads
    factor = HEAD_DIM ** -0.5 * math.log2(math.e)
    cp = lax.axis_index("cp")
    chip, core = cp // 2, lax.rem(cp, 2)
    chips = count // 2
    y = lax.rem(chip, RING_Y)
    row = chip - y

    def core_of(which_chip):
        return which_chip * 2 + core

    partner = chip * 2 + (1 - core)
    has_after, has_before = chip + 1 < chips, chip >= 1
    after, before = core_of(jnp.minimum(chip + 1, chips - 1)), core_of(jnp.maximum(chip - 1, 0))
    three_down = core_of(row + lax.rem(y + RING_Y - 3, RING_Y))
    goes_down = chip + 3 < chips
    relay_owner = row + lax.rem(y + 3, RING_Y)
    three_up = core_of(relay_owner)
    has_relay = relay_owner + 3 < chips
    relay_last = relay_owner + 4 == chips
    relay_to = core_of(jnp.minimum(relay_owner + 4, chips - 1))
    relay_slot = jnp.where(relay_last, 5, LANDED)
    owner = jnp.maximum(chip - 4, 0)
    owner_y = lax.rem(owner, RING_Y)
    relay_from = core_of(owner - owner_y + lax.rem(owner_y + RING_Y - 3, RING_Y))
    has_landed = chip >= 4
    is_last = chip + 1 == chips
    last_from = core_of(chips - 4 - (chips - 4) % RING_Y + ((chips - 4) % RING_Y + RING_Y - 3) % RING_Y)

    def holds(slot, me):
        if slot == RELAY:
            return has_relay
        if slot == LANDED or (slot == FAR and me == 0):
            return has_landed
        if slot == FAR or slot == OWN:
            return chip >= 0
        return chip >= slot // 2 + 1

    def piece(slot, p):
        return kv.at[slot, p % 2, p // 2]

    def remote(src, dst, send, recv, to):
        return pltpu.make_async_remote_copy(
            src_ref=src, dst_ref=dst, send_sem=send, recv_sem=recv,
            device_id={"cp": to}, device_id_type=pl.DeviceIdType.MESH)

    loads = []
    for p in range(4):
        source = (k_hbm, v_hbm)[p % 2].at[:, pl.ds(p // 2 * HEAD_DIM, HEAD_DIM)]
        loads.append(pltpu.make_async_copy(source, piece(OWN, p), load_sem.at[p]))
    loads.append(pltpu.make_async_copy(q_hbm, q_in, load_sem.at[4]))
    for copy in loads:
        copy.start()

    barrier = pltpu.get_barrier_semaphore()

    def greet(peers):
        for known, device in peers:
            @pl.when(known)
            def _():
                pl.semaphore_signal(barrier, inc=1, device_id={"cp": device}, device_id_type=pl.DeviceIdType.MESH)
        pl.semaphore_wait(barrier, sum(known.astype(jnp.int32) for known, _ in peers))

    near = ((chip >= 0, partner), (has_after, after), (has_before, before))

    @pl.when(core == 0)
    def _():
        greet(near)

    @pl.when(core == 1)
    def _():
        greet(near + ((goes_down, three_down), (has_relay, three_up), (has_relay, relay_to),
                      (has_landed, relay_from), (is_last, last_from)))

    for copy in loads[:4]:
        copy.wait()

    def own_send(lane, p):
        to, slot = ((after, core), (partner, FAR), (three_down, RELAY))[lane]
        return (has_after, chip >= 0, goes_down)[lane], remote(
            piece(OWN, p), piece(slot, p), own_sem.at[lane, p], recv_sem.at[slot, p], to)

    def relay(slot, p):
        to, target = {0: (after, 2), 1: (after, 3), 2: (after, 4), RELAY: (relay_to, relay_slot), LANDED: (before, 5)}[slot]
        known = holds(slot, 0) & has_after if slot in (0, 1, 2) else holds(slot, 1)
        return known, remote(piece(slot, p), piece(target, p), relay_sem.at[slot, p], recv_sem.at[target, p], to)

    def cross(slot, p):
        target = FAR if slot == LANDED else slot
        return holds(slot, 1), remote(piece(slot, p), piece(target, p), cross_sem.at[slot, p], recv_sem.at[target, p], partner)

    def if_known(known_and_copy, act):
        known, copy = known_and_copy

        @pl.when(known)
        def _():
            act(copy)

    def event(me, slot, pieces):
        for p in pieces:
            @pl.when(holds(slot, me))
            def _():
                remote(piece(slot, p), piece(slot, p), cross_sem.at[slot, p], recv_sem.at[slot, p], partner).wait_recv()
                if slot in RELAYED[me]:
                    if_known(relay(slot, p), lambda copy: copy.start())
                if slot in CROSSED[me]:
                    cross(slot, p)[1].start()

    for me in (0, 1):
        @pl.when(core == me)
        def _():
            for p in range(4):
                for lane in OWN_LANES[me]:
                    if_known(own_send(lane, p), lambda copy: copy.start())

    for slot in range(FAR + 1):
        @pl.when(~(holds(slot, 1) if slot < FAR else (holds(FAR, 0) | (core == 1))))
        def _():
            kv[slot] = jnp.zeros(kv.shape[1:], kv.dtype)

    query_pos = cp * toks + lax.broadcasted_iota(jnp.int32, (1, toks), 1)
    starts = jnp.zeros((1, toks), jnp.int32)
    position = jnp.int32(0)
    for doc in range(lengths.shape[0]):
        starts = jnp.where(query_pos >= position, position, starts)
        position = position + lengths[doc]
    first_live[...] = starts

    loads[4].wait()
    for h in range(heads):
        qt[h // group, h % group] = q_in[:, h * HEAD_DIM : (h + 1) * HEAD_DIM].T
    acc[...] = jnp.zeros_like(acc)
    total[...] = jnp.zeros_like(total)
    top[...] = jnp.full_like(top, MASKED)
    old_top[...] = jnp.zeros_like(old_top)
    new_top[...] = jnp.zeros_like(new_top)
    rescale[...] = jnp.ones_like(rescale)
    for half in range(2):
        for k in range(PAIR):
            scores[half, k] = jnp.full(scores.shape[2:], MASKED, jnp.float32)
            weights[half, k] = jnp.zeros(weights.shape[2:], weights.dtype)

    def where_is(step):
        in_pairs = jnp.where(core == 0, jnp.where(step < 10, step - 2, step - 4), step - 4)
        far = jnp.where(core == 0, (step == 10) | (step == 11), (step == 2) | (step == 3))
        single = far | (step < 2)
        in_pairs = jnp.maximum(in_pairs, 0)
        distance = in_pairs // 4
        parity = lax.rem(in_pairs, 2)
        slot = jnp.where(step < 2, OWN, jnp.where(far, FAR, 2 * distance + parity))
        head = jnp.where(single, lax.rem(step, 2), lax.rem(in_pairs, 4) // 2)
        far_block = jnp.where(core == 0, 2 * chip - 7, 2 * chip)
        block = jnp.where(step < 2, cp, jnp.where(far, far_block, 2 * (chip - distance - 1) + parity))
        return slot, head, block

    def score(slot, head, half):
        keys = kv[slot, 0, head]
        side = lax.rem(slot, 2)
        for k in range(PAIR):
            h = half * PAIR + k
            found = jnp.dot(keys, qt[head, h], preferred_element_type=jnp.float32) + bias[side]
            scores[half, k] = found
            old = top[head, pl.ds(h, 1)]
            new = jnp.maximum(old, jnp.max(found, axis=0, keepdims=True))
            top[head, pl.ds(h, 1)] = new
            old_top[half, pl.ds(k, 1)] = old
            new_top[half, pl.ds(k, 1)] = new

    def weigh(head, half):
        for k in range(PAIR):
            h = half * PAIR + k
            new = new_top[half, pl.ds(k, 1)]
            shrink = jnp.exp2((old_top[half, pl.ds(k, 1)] - new) * factor)
            found = jnp.exp2((scores[half, k] - new) * factor)
            weights[half, k] = found.astype(jnp.bfloat16)
            rescale[half, pl.ds(k, 1)] = shrink
            total[head, pl.ds(h, 1)] = total[head, pl.ds(h, 1)] * shrink + jnp.sum(found, axis=0, keepdims=True)

    def gather(head, half, values):
        for k in range(PAIR):
            h = half * PAIR + k
            acc[head, h] = acc[head, h] * rescale[half, pl.ds(k, 1)] + jnp.dot(
                values, weights[half, k], preferred_element_type=jnp.float32)

    def step_body(step, carry):
        for quarter in range(STEPS // 4):
            @pl.when(step // 4 == quarter)
            def _():
                for s in range(4 * quarter, 4 * quarter + 4):
                    for me in (0, 1):
                        if s in AHEAD[me]:
                            @pl.when((step == s) & (core == me))
                            def _():
                                for slot, pieces in AHEAD[me][s]:
                                    event(me, slot, pieces)

        slot, head, block = where_is(step)
        last_slot, last_head, _ = where_is(jnp.maximum(step - 1, 0))

        @pl.when(head == 0)
        def _():
            key_pos = block * toks + lax.broadcasted_iota(jnp.int32, (toks, toks), 0)
            live = (key_pos >= first_live[...]) & (key_pos <= cp * toks + lax.broadcasted_iota(jnp.int32, (toks, toks), 1))
            bias[lax.rem(slot, 2)] = jnp.where(live, 0.0, MASKED)

        values = kv[last_slot, 1, last_head].T
        score(slot, head, 0)
        weigh(last_head, 1)
        gather(last_head, 0, values)
        score(slot, head, 1)
        weigh(head, 0)
        gather(last_head, 1, values)
        return carry

    lax.fori_loop(0, STEPS, step_body, 0)
    last_slot, last_head, _ = where_is(jnp.int32(STEPS - 1))
    values = kv[last_slot, 1, last_head].T
    weigh(last_head, 1)
    gather(last_head, 0, values)
    gather(last_head, 1, values)

    stores = []
    for h in range(heads):
        columns = slice(h * HEAD_DIM, (h + 1) * HEAD_DIM)
        share = 1.0 / total[h // group, h % group : h % group + 1]
        out_v[:, columns] = (acc[h // group, h % group] * share).astype(out_v.dtype).T
        if h % group == group - 1:
            columns = pl.ds((h + 1 - group) * HEAD_DIM, group * HEAD_DIM)
            copy = pltpu.make_async_copy(out_v.at[:, columns], out_hbm.at[:, columns], out_sem.at[h // group])
            copy.start()
            stores.append(copy)
    for me in (0, 1):
        @pl.when(core == me)
        def _():
            for p in range(4):
                for lane in OWN_LANES[me]:
                    if_known(own_send(lane, p), lambda copy: copy.wait_send())
                for slot in RELAYED[me]:
                    if_known(relay(slot, p), lambda copy: copy.wait_send())
                for slot in CROSSED[me]:
                    if_known(cross(slot, p), lambda copy: copy.wait_send())
    for copy in stores:
        copy.wait()


def body(count, queries, keys, values, lengths):
    toks, wide = queries.shape
    heads = wide // HEAD_DIM
    kv_heads = keys.shape[1] // HEAD_DIM
    group = heads // kv_heads
    return pl.pallas_call(
        functools.partial(kernel, count),
        out_shape=jax.ShapeDtypeStruct((toks, wide), jnp.bfloat16),
        in_specs=[pl.BlockSpec(memory_space=pl.ANY)] * 3 + [pl.BlockSpec(memory_space=pltpu.SMEM)],
        out_specs=pl.BlockSpec(memory_space=pl.ANY),
        scratch_shapes=[
            pltpu.VMEM((SLOTS, 2, kv_heads, toks, HEAD_DIM), jnp.bfloat16),
            pltpu.VMEM((toks, wide), jnp.bfloat16),
            pltpu.VMEM((kv_heads, group, HEAD_DIM, toks), jnp.bfloat16),
            pltpu.VMEM((kv_heads, group, HEAD_DIM, toks), jnp.float32),
            pltpu.VMEM((kv_heads, group, toks), jnp.float32),
            pltpu.VMEM((kv_heads, group, toks), jnp.float32),
            pltpu.VMEM((1, toks), jnp.int32),
            pltpu.VMEM((2, toks, toks), jnp.float32),
            pltpu.VMEM((2, PAIR, toks, toks), jnp.float32),
            pltpu.VMEM((2, PAIR, toks, toks), jnp.bfloat16),
            pltpu.VMEM((2, PAIR, toks), jnp.float32),
            pltpu.VMEM((2, PAIR, toks), jnp.float32),
            pltpu.VMEM((2, PAIR, toks), jnp.float32),
            pltpu.VMEM((toks, wide), jnp.bfloat16),
            pltpu.SemaphoreType.DMA((5,)),
            pltpu.SemaphoreType.DMA((2,)),
            pltpu.SemaphoreType.DMA((SLOTS, 4)),
            pltpu.SemaphoreType.DMA((3, 4)),
            pltpu.SemaphoreType.DMA((SLOTS, 4)),
            pltpu.SemaphoreType.DMA((SLOTS, 4)),
        ],
        compiler_params=pltpu.CompilerParams(collective_id=0, has_side_effects=True),
    )(queries, keys, values, lengths)


def solution(mesh):
    in_specs = (P("cp", "tp"), P("cp", "tp"), P("cp", "tp"), P())
    return jax.shard_map(functools.partial(body, mesh.shape["cp"]), mesh=mesh, in_specs=in_specs,
                         out_specs=P("cp", "tp"), check_vma=False)
```

```python
import functools
import math

import jax
import jax.numpy as jnp
from jax import lax
from jax.experimental import pallas as pl
from jax.experimental.pallas import tpu as pltpu
from jax.sharding import PartitionSpec as P

HEAD_DIM = 128
RING_Y = 8
PAIR = 2
MASKED = -1e30
FAR = 6
LANDED = 7
RELAY = 8
OWN = 9
SPARE = 10
SLOTS = 11
FIRST, SECOND = (0, 1), (2, 3)
STEPS = 14
SHORT_WAY = (3,)
AHEAD = (
    {0: ((0, FIRST),), 1: ((1, FIRST),), 2: ((0, SECOND),), 3: ((1, SECOND),),
     4: ((2, FIRST),), 5: ((3, FIRST),), 6: ((2, SECOND),), 7: ((3, SECOND),),
     8: ((FAR, FIRST),), 9: ((FAR, SECOND),),
     10: ((4, FIRST),), 11: ((5, FIRST),), 12: ((4, SECOND),), 13: ((5, SECOND),)},
    {0: ((FAR, FIRST),), 1: ((FAR, SECOND),),
     2: ((1, FIRST), (RELAY, (0,)), (SPARE, (0,)), (0, FIRST)), 4: ((RELAY, (1,)), (SPARE, (1,)), (1, SECOND), (0, SECOND)),
     6: ((RELAY, (2,)), (SPARE, (2, 3)), (3, FIRST), (2, FIRST)),
     8: ((RELAY, (3,)), (LANDED, (0, 1)), (3, SECOND), (LANDED, (2, 3)), (2, SECOND)),
     10: ((5, FIRST), (4, FIRST)), 12: ((5, SECOND), (4, SECOND))},
)
OWN_LANES = ((0, 1), (0, 2, 3))
RELAYED = ((0, 2), (1, 3, RELAY, LANDED, SPARE))
CROSSED = ((0, 2, 4), (1, 3, LANDED, 5))


def kernel(count, q_hbm, k_hbm, v_hbm, lengths, out_hbm,
           kv, q_in, qt, acc, top, total, bounds, key_mask, query_mask, scores, weights, old_top, new_top, rescale, out_v,
           load_sem, out_sem, recv_sem, own_sem, relay_sem, cross_sem):
    toks = q_in.shape[0]
    kv_heads = kv.shape[2]
    heads = q_in.shape[1] // HEAD_DIM
    group = heads // kv_heads
    factor = HEAD_DIM ** -0.5 * math.log2(math.e)
    cp = lax.axis_index("cp")
    chip, core = cp // 2, lax.rem(cp, 2)
    chips = count // 2
    y = lax.rem(chip, RING_Y)
    row = chip - y

    def core_of(which_chip):
        return which_chip * 2 + core

    partner = chip * 2 + (1 - core)
    has_after, has_before = chip + 1 < chips, chip >= 1
    after, before = core_of(jnp.minimum(chip + 1, chips - 1)), core_of(jnp.maximum(chip - 1, 0))
    goes_down = chip + 4 < chips
    down = core_of(jnp.minimum(row + jnp.where(y >= 4, RING_Y, 0), chips - RING_Y) + lax.rem(y + RING_Y - 3, RING_Y))
    reader = row + lax.rem(y + RING_Y - 1, RING_Y)
    has_relay = reader >= 4
    relay_to, relay_owner = core_of(reader), core_of(jnp.maximum(reader - 4, 0))
    relay_from = core_of(row + lax.rem(y + 1, RING_Y))
    has_landed = chip >= 4
    owner_chip, reader_chip = chips - 4, chips - 1
    between_chip = owner_chip - owner_chip % RING_Y + (owner_chip + RING_Y - 3) % RING_Y
    is_owner, is_between, is_reader = chip == owner_chip, chip == between_chip, chip == reader_chip

    def holds(slot, me):
        if slot == RELAY:
            return has_relay
        if slot == SPARE:
            return is_between
        if slot == LANDED or (slot == FAR and me == 0):
            return has_landed
        if slot == FAR or slot == OWN:
            return chip >= 0
        return chip >= slot // 2 + 1

    def piece(slot, p):
        return kv.at[slot, p % 2, p // 2]

    def remote(src, dst, send, recv, to):
        return pltpu.make_async_remote_copy(
            src_ref=src, dst_ref=dst, send_sem=send, recv_sem=recv,
            device_id={"cp": to}, device_id_type=pl.DeviceIdType.MESH)

    loads = []
    for p in range(4):
        source = (k_hbm, v_hbm)[p % 2].at[:, pl.ds(p // 2 * HEAD_DIM, HEAD_DIM)]
        loads.append(pltpu.make_async_copy(source, piece(OWN, p), load_sem.at[p]))
    loads.append(pltpu.make_async_copy(q_hbm, q_in, load_sem.at[4]))
    for copy in loads:
        copy.start()

    barrier = pltpu.get_barrier_semaphore()

    def greet(peers):
        for known, device in peers:
            @pl.when(known)
            def _():
                pl.semaphore_signal(barrier, inc=1, device_id={"cp": device}, device_id_type=pl.DeviceIdType.MESH)
        pl.semaphore_wait(barrier, sum(known.astype(jnp.int32) for known, _ in peers))

    near = ((chip >= 0, partner), (has_after, after), (has_before, before))

    @pl.when(core == 0)
    def _():
        greet(near)

    @pl.when(core == 1)
    def _():
        greet(near + ((goes_down, down), (has_relay, relay_owner), (has_relay, relay_to), (has_landed, relay_from),
                      (is_owner | is_reader, core_of(between_chip)),
                      (is_between, core_of(owner_chip)), (is_between, core_of(reader_chip))))

    for copy in loads[:4]:
        copy.wait()

    def own_send(lane, p):
        to, slot = ((after, core), (partner, FAR), (down, RELAY), (core_of(between_chip), SPARE))[lane]
        return (has_after, chip >= 0, goes_down, is_owner)[lane], remote(
            piece(OWN, p), piece(slot, p), own_sem.at[lane, p], recv_sem.at[slot, p], to)

    def relay(slot, p):
        to, target = {0: (after, 2), 1: (after, 3), 2: (after, 4), 3: (after, 5),
                      RELAY: (relay_to, LANDED), LANDED: (before, 5), SPARE: (core_of(reader_chip), 5)}[slot]
        known = holds(slot, 1)
        if slot < FAR:
            known = known & has_after
        return known, remote(piece(slot, p), piece(target, p), relay_sem.at[slot, p], recv_sem.at[target, p], to)

    def relayed(me, slot, p):
        if slot == 3 and p not in SHORT_WAY or slot in (LANDED, SPARE) and p in SHORT_WAY:
            return False
        return slot in RELAYED[me]

    def cross(slot, p):
        target = FAR if slot == LANDED else slot
        return holds(slot, 1), remote(piece(slot, p), piece(target, p), cross_sem.at[slot, p], recv_sem.at[target, p], partner)

    def if_known(known_and_copy, act):
        known, copy = known_and_copy

        @pl.when(known)
        def _():
            act(copy)

    def event(me, slot, pieces):
        for p in pieces:
            @pl.when(holds(slot, me))
            def _():
                remote(piece(slot, p), piece(slot, p), cross_sem.at[slot, p], recv_sem.at[slot, p], partner).wait_recv()
                if relayed(me, slot, p):
                    if_known(relay(slot, p), lambda copy: copy.start())
                if slot in CROSSED[me]:
                    cross(slot, p)[1].start()

    for me in (0, 1):
        @pl.when(core == me)
        def _():
            for p in range(4):
                for lane in OWN_LANES[me]:
                    if_known(own_send(lane, p), lambda copy: copy.start())

    for slot in range(FAR + 1):
        @pl.when(~(holds(slot, 1) if slot < FAR else (holds(FAR, 0) | (core == 1))))
        def _():
            kv[slot] = jnp.zeros(kv.shape[1:], kv.dtype)

    feature = lax.broadcasted_iota(jnp.int32, (1, HEAD_DIM), 1)
    begins = jnp.where(feature == lengths.shape[0], -(1 << 20), jnp.full((1, HEAD_DIM), 1 << 20, jnp.int32))
    ends = jnp.zeros((1, HEAD_DIM), jnp.int32)
    position = jnp.int32(0)
    for doc in range(lengths.shape[0]):
        begins = jnp.where(feature == doc, position, begins)
        position = position + lengths[doc]
        ends = jnp.where(feature == doc, position, ends)
    bounds[0:1] = begins.astype(jnp.float32)
    bounds[1:2] = ends.astype(jnp.float32)
    begins = jnp.broadcast_to(bounds[0:1], (HEAD_DIM, HEAD_DIM)).T
    ends = jnp.broadcast_to(bounds[1:2], (HEAD_DIM, HEAD_DIM)).T
    for tile in range(toks // HEAD_DIM):
        query_pos = (cp * toks + tile * HEAD_DIM + lax.broadcasted_iota(jnp.int32, (HEAD_DIM, HEAD_DIM), 1)).astype(jnp.float32)
        outside = (query_pos < begins) | (query_pos >= ends)
        outside = outside & (lax.broadcasted_iota(jnp.int32, (HEAD_DIM, HEAD_DIM), 0) <= lengths.shape[0])
        query_mask[:, tile * HEAD_DIM : (tile + 1) * HEAD_DIM] = jnp.where(outside, MASKED, 0.0).astype(jnp.bfloat16)

    def mark(side, block):
        key_pos = (block * toks + lax.broadcasted_iota(jnp.int32, (toks, HEAD_DIM), 0)).astype(jnp.float32)
        inside = (key_pos >= bounds[0:1]) & (key_pos < bounds[1:2])
        key_mask[side] = jnp.where(inside, 1.0, 0.0).astype(jnp.bfloat16)

    def product(keys, side, head, h):
        return jnp.dot(
            jnp.concatenate([keys, key_mask[side]], axis=1),
            jnp.concatenate([qt[head, h], query_mask[...]], axis=0),
            preferred_element_type=jnp.float32)

    loads[4].wait()
    for h in range(heads):
        qt[h // group, h % group] = q_in[:, h * HEAD_DIM : (h + 1) * HEAD_DIM].T
    old_top[...] = jnp.zeros_like(old_top)
    new_top[...] = jnp.zeros_like(new_top)
    rescale[...] = jnp.ones_like(rescale)
    for k in range(PAIR):
        scores[1, k] = jnp.full(scores.shape[2:], MASKED, jnp.float32)
        for half in range(2):
            weights[half, k] = jnp.zeros(weights.shape[2:], weights.dtype)

    mark(1, cp)

    def own_body(head, carry):
        keys = kv[OWN, 0, head]
        values = kv[OWN, 1, head].T
        causal = lax.broadcasted_iota(jnp.int32, (toks, toks), 0) <= lax.broadcasted_iota(jnp.int32, (toks, toks), 1)
        for h in range(group):
            found = jnp.where(causal, product(keys, 1, head, h), MASKED)
            new = jnp.max(found, axis=0, keepdims=True)
            found = jnp.exp2((found - new) * factor)
            top[head, pl.ds(h, 1)] = new
            total[head, pl.ds(h, 1)] = jnp.sum(found, axis=0, keepdims=True)
            acc[head, h] = jnp.dot(values, found.astype(jnp.bfloat16), preferred_element_type=jnp.float32)
        return carry

    lax.fori_loop(0, kv_heads, own_body, 0)

    def where_is(step):
        in_pairs = jnp.where(core == 0, jnp.where(step < 8, step, step - 2), step - 2)
        far = jnp.where(core == 0, (step == 8) | (step == 9), step < 2)
        in_pairs = jnp.maximum(in_pairs, 0)
        distance = in_pairs // 4
        parity = lax.rem(in_pairs, 2)
        slot = jnp.where(far, FAR, 2 * distance + parity)
        head = jnp.where(far, lax.rem(step, 2), lax.rem(in_pairs, 4) // 2)
        far_block = jnp.where(core == 0, 2 * chip - 7, 2 * chip)
        block = jnp.where(far, far_block, 2 * (chip - distance - 1) + parity)
        return slot, head, block

    def score(slot, head, half):
        keys = kv[slot, 0, head]
        side = lax.rem(slot, 2)
        for k in range(PAIR):
            h = half * PAIR + k
            found = product(keys, side, head, h)
            scores[half, k] = found
            old = top[head, pl.ds(h, 1)]
            new = jnp.maximum(old, jnp.max(found, axis=0, keepdims=True))
            top[head, pl.ds(h, 1)] = new
            old_top[half, pl.ds(k, 1)] = old
            new_top[half, pl.ds(k, 1)] = new

    def weigh(head, half):
        for k in range(PAIR):
            h = half * PAIR + k
            new = new_top[half, pl.ds(k, 1)]
            shrink = jnp.exp2((old_top[half, pl.ds(k, 1)] - new) * factor)
            found = jnp.exp2((scores[half, k] - new) * factor)
            weights[half, k] = found.astype(jnp.bfloat16)
            rescale[half, pl.ds(k, 1)] = shrink
            total[head, pl.ds(h, 1)] = total[head, pl.ds(h, 1)] * shrink + jnp.sum(found, axis=0, keepdims=True)

    def gather(head, half, values):
        for k in range(PAIR):
            h = half * PAIR + k
            acc[head, h] = acc[head, h] * rescale[half, pl.ds(k, 1)] + jnp.dot(
                values, weights[half, k], preferred_element_type=jnp.float32)

    def step_body(step, carry):
        for quarter in range((STEPS + 3) // 4):
            @pl.when(step // 4 == quarter)
            def _():
                for s in range(4 * quarter, 4 * quarter + 4):
                    for me in (0, 1):
                        if s in AHEAD[me]:
                            @pl.when((step == s) & (core == me))
                            def _():
                                for slot, pieces in AHEAD[me][s]:
                                    event(me, slot, pieces)

        slot, head, block = where_is(step)
        last_slot, last_head, _ = where_is(jnp.maximum(step - 1, 0))

        @pl.when(head == 0)
        def _():
            mark(lax.rem(slot, 2), block)

        values = kv[last_slot, 1, last_head].T
        weigh(last_head, 1)
        score(slot, head, 0)
        gather(last_head, 0, values)
        score(slot, head, 1)
        gather(last_head, 1, values)
        weigh(head, 0)
        return carry

    lax.fori_loop(0, STEPS, step_body, 0)
    last_slot, last_head, _ = where_is(jnp.int32(STEPS - 1))
    values = kv[last_slot, 1, last_head].T
    weigh(last_head, 1)
    gather(last_head, 0, values)
    gather(last_head, 1, values)

    stores = []
    for h in range(heads):
        columns = slice(h * HEAD_DIM, (h + 1) * HEAD_DIM)
        share = 1.0 / total[h // group, h % group : h % group + 1]
        out_v[:, columns] = (acc[h // group, h % group] * share).astype(out_v.dtype).T
        if h % group == group - 1:
            columns = pl.ds((h + 1 - group) * HEAD_DIM, group * HEAD_DIM)
            copy = pltpu.make_async_copy(out_v.at[:, columns], out_hbm.at[:, columns], out_sem.at[h // group])
            copy.start()
            stores.append(copy)
    for me in (0, 1):
        @pl.when(core == me)
        def _():
            for p in range(4):
                for lane in OWN_LANES[me]:
                    if_known(own_send(lane, p), lambda copy: copy.wait_send())
                for slot in RELAYED[me]:
                    if relayed(me, slot, p):
                        if_known(relay(slot, p), lambda copy: copy.wait_send())
                for slot in CROSSED[me]:
                    if_known(cross(slot, p), lambda copy: copy.wait_send())
    for copy in stores:
        copy.wait()


def body(count, queries, keys, values, lengths):
    toks, wide = queries.shape
    heads = wide // HEAD_DIM
    kv_heads = keys.shape[1] // HEAD_DIM
    group = heads // kv_heads
    return pl.pallas_call(
        functools.partial(kernel, count),
        out_shape=jax.ShapeDtypeStruct((toks, wide), jnp.bfloat16),
        in_specs=[pl.BlockSpec(memory_space=pl.ANY)] * 3 + [pl.BlockSpec(memory_space=pltpu.SMEM)],
        out_specs=pl.BlockSpec(memory_space=pl.ANY),
        scratch_shapes=[
            pltpu.VMEM((SLOTS, 2, kv_heads, toks, HEAD_DIM), jnp.bfloat16),
            pltpu.VMEM((toks, wide), jnp.bfloat16),
            pltpu.VMEM((kv_heads, group, HEAD_DIM, toks), jnp.bfloat16),
            pltpu.VMEM((kv_heads, group, HEAD_DIM, toks), jnp.float32),
            pltpu.VMEM((kv_heads, group, toks), jnp.float32),
            pltpu.VMEM((kv_heads, group, toks), jnp.float32),
            pltpu.VMEM((2, HEAD_DIM), jnp.float32),
            pltpu.VMEM((2, toks, HEAD_DIM), jnp.bfloat16),
            pltpu.VMEM((HEAD_DIM, toks), jnp.bfloat16),
            pltpu.VMEM((2, PAIR, toks, toks), jnp.float32),
            pltpu.VMEM((2, PAIR, toks, toks), jnp.bfloat16),
            pltpu.VMEM((2, PAIR, toks), jnp.float32),
            pltpu.VMEM((2, PAIR, toks), jnp.float32),
            pltpu.VMEM((2, PAIR, toks), jnp.float32),
            pltpu.VMEM((toks, wide), jnp.bfloat16),
            pltpu.SemaphoreType.DMA((5,)),
            pltpu.SemaphoreType.DMA((2,)),
            pltpu.SemaphoreType.DMA((SLOTS, 4)),
            pltpu.SemaphoreType.DMA((4, 4)),
            pltpu.SemaphoreType.DMA((SLOTS, 4)),
            pltpu.SemaphoreType.DMA((SLOTS, 4)),
        ],
        compiler_params=pltpu.CompilerParams(collective_id=0, has_side_effects=True),
    )(queries, keys, values, lengths)


def solution(mesh):
    in_specs = (P("cp", "tp"), P("cp", "tp"), P("cp", "tp"), P())
    return jax.shard_map(functools.partial(body, mesh.shape["cp"]), mesh=mesh, in_specs=in_specs,
                         out_specs=P("cp", "tp"), check_vma=False)
```

```python
import functools
import math

import jax
import jax.numpy as jnp
from jax import lax
from jax.experimental import pallas as pl
from jax.experimental.pallas import tpu as pltpu
from jax.sharding import PartitionSpec as P

HEAD_DIM = 128
RING_Y = 8
PAIR = 2
MASKED = -1e30
TILE = 256
FAR = 6
LANDED = 7
RELAY = 8
OWN = 9
SPARE = 10
SLOTS = 11
FIRST, SECOND = (0, 1), (2, 3)
STEPS = 14
SHORT_WAY = (2, 3)
AHEAD = (
    {0: ((0, FIRST),), 1: ((1, FIRST),), 2: ((0, SECOND),), 3: ((1, SECOND),),
     4: ((2, FIRST),), 5: ((3, FIRST),), 6: ((2, SECOND),), 7: ((3, SECOND),),
     8: ((FAR, FIRST),), 9: ((FAR, SECOND),),
     10: ((4, (0,)), (5, FIRST)), 11: ((4, (1,)),), 12: ((5, SECOND), (4, (2,))), 13: ((4, (3,)),)},
    {0: ((FAR, FIRST),), 1: ((FAR, SECOND),),
     2: ((1, FIRST), (RELAY, (0,)), (SPARE, (0,)), (0, FIRST)),
     4: ((RELAY, (1,)), (SPARE, (1,)), (1, SECOND), (0, SECOND)),
     6: ((RELAY, (2,)), (SPARE, (2, 3)), (3, FIRST), (2, FIRST)),
     8: ((RELAY, (3,)), (LANDED, (0, 1)), (3, (2,)), (LANDED, (2,)), (3, (3,)), (LANDED, (3,)), (2, SECOND)),
     10: ((5, (0,)), (5, (2,)), (5, (1,))), 11: ((5, (3,)), (4, FIRST)), 13: ((4, SECOND),)},
)
OWN_LANES = ((0, 1), (0, 2, 3))
RELAYED = ((0, 2), (1, 3, RELAY, LANDED, SPARE))
CROSSED = ((0, 2, 4), (1, 3, LANDED, 5))


def kernel(count, q_hbm, k_hbm, v_hbm, lengths, out,
           kv, q_in, qt, acc, top, total, bounds, key_mask, query_mask, scores, weights, old_top, new_top, rescale,
           load_sem, recv_sem, own_sem, relay_sem, cross_sem):
    toks = q_in.shape[0]
    kv_heads = kv.shape[2]
    heads = q_in.shape[1] // HEAD_DIM
    group = heads // kv_heads
    factor = HEAD_DIM ** -0.5 * math.log2(math.e)
    cp = lax.axis_index("cp")
    chip, core = cp // 2, lax.rem(cp, 2)
    chips = count // 2
    y = lax.rem(chip, RING_Y)
    row = chip - y

    def core_of(which_chip):
        return which_chip * 2 + core

    partner = chip * 2 + (1 - core)
    has_after, has_before = chip + 1 < chips, chip >= 1
    after, before = core_of(jnp.minimum(chip + 1, chips - 1)), core_of(jnp.maximum(chip - 1, 0))
    goes_down = chip + 4 < chips
    down = core_of(jnp.minimum(row + jnp.where(y >= 4, RING_Y, 0), chips - RING_Y) + lax.rem(y + RING_Y - 3, RING_Y))
    reader = row + lax.rem(y + RING_Y - 1, RING_Y)
    has_relay = reader >= 4
    relay_to, relay_owner = core_of(reader), core_of(jnp.maximum(reader - 4, 0))
    relay_from = core_of(row + lax.rem(y + 1, RING_Y))
    has_landed = chip >= 4
    owner_chip, reader_chip = chips - 4, chips - 1
    between_chip = owner_chip - owner_chip % RING_Y + (owner_chip + RING_Y - 3) % RING_Y
    is_owner, is_between, is_reader = chip == owner_chip, chip == between_chip, chip == reader_chip

    def holds(slot, me):
        if slot == RELAY:
            return has_relay
        if slot == SPARE:
            return is_between
        if slot == LANDED or (slot == FAR and me == 0):
            return has_landed
        if slot == FAR or slot == OWN:
            return chip >= 0
        return chip >= slot // 2 + 1

    def piece(slot, p):
        return kv.at[slot, p % 2, p // 2]

    def remote(src, dst, send, recv, to):
        return pltpu.make_async_remote_copy(
            src_ref=src, dst_ref=dst, send_sem=send, recv_sem=recv,
            device_id={"cp": to}, device_id_type=pl.DeviceIdType.MESH)

    loads = []
    for p in range(4):
        source = (k_hbm, v_hbm)[p % 2].at[:, pl.ds(p // 2 * HEAD_DIM, HEAD_DIM)]
        loads.append(pltpu.make_async_copy(source, piece(OWN, p), load_sem.at[p]))
    loads.append(pltpu.make_async_copy(q_hbm, q_in, load_sem.at[4]))
    for copy in loads:
        copy.start()

    barrier = pltpu.get_barrier_semaphore()

    def greet(peers):
        for known, device in peers:
            @pl.when(known)
            def _():
                pl.semaphore_signal(barrier, inc=1, device_id={"cp": device}, device_id_type=pl.DeviceIdType.MESH)
        pl.semaphore_wait(barrier, sum(known.astype(jnp.int32) for known, _ in peers))

    near = ((chip >= 0, partner), (has_after, after), (has_before, before))

    @pl.when(core == 0)
    def _():
        greet(near)

    @pl.when(core == 1)
    def _():
        greet(near + ((goes_down, down), (has_relay, relay_owner), (has_relay, relay_to), (has_landed, relay_from),
                      (is_owner | is_reader, core_of(between_chip)),
                      (is_between, core_of(owner_chip)), (is_between, core_of(reader_chip))))

    for copy in loads[:4]:
        copy.wait()

    def own_send(lane, p):
        to, slot = ((after, core), (partner, FAR), (down, RELAY), (core_of(between_chip), SPARE))[lane]
        return (has_after, chip >= 0, goes_down, is_owner)[lane], remote(
            piece(OWN, p), piece(slot, p), own_sem.at[lane, p], recv_sem.at[slot, p], to)

    def relay(slot, p):
        to, target = {0: (after, 2), 1: (after, 3), 2: (after, 4), 3: (after, 5),
                      RELAY: (relay_to, LANDED), LANDED: (before, 5), SPARE: (core_of(reader_chip), 5)}[slot]
        known = holds(slot, 1)
        if slot < FAR:
            known = known & has_after
        return known, remote(piece(slot, p), piece(target, p), relay_sem.at[slot, p], recv_sem.at[target, p], to)

    def relayed(me, slot, p):
        if slot == 3 and p not in SHORT_WAY or slot in (LANDED, SPARE) and p in SHORT_WAY:
            return False
        return slot in RELAYED[me]

    def cross(slot, p):
        target = FAR if slot == LANDED else slot
        return holds(slot, 1), remote(piece(slot, p), piece(target, p), cross_sem.at[slot, p], recv_sem.at[target, p], partner)

    def if_known(known_and_copy, act):
        known, copy = known_and_copy

        @pl.when(known)
        def _():
            act(copy)

    def event(me, slot, pieces):
        for p in pieces:
            @pl.when(holds(slot, me))
            def _():
                remote(piece(slot, p), piece(slot, p), cross_sem.at[slot, p], recv_sem.at[slot, p], partner).wait_recv()
                if relayed(me, slot, p):
                    if_known(relay(slot, p), lambda copy: copy.start())
                if slot in CROSSED[me]:
                    cross(slot, p)[1].start()

    for me in (0, 1):
        @pl.when(core == me)
        def _():
            for p in range(4):
                for lane in OWN_LANES[me]:
                    if_known(own_send(lane, p), lambda copy: copy.start())

    for slot in range(FAR + 1):
        @pl.when(~(holds(slot, 1) if slot < FAR else (holds(FAR, 0) | (core == 1))))
        def _():
            kv[slot] = jnp.zeros(kv.shape[1:], kv.dtype)

    feature = lax.broadcasted_iota(jnp.int32, (1, HEAD_DIM), 1)
    begins = jnp.where(feature == lengths.shape[0], -(1 << 20), jnp.full((1, HEAD_DIM), 1 << 20, jnp.int32))
    ends = jnp.zeros((1, HEAD_DIM), jnp.int32)
    position = jnp.int32(0)
    for doc in range(lengths.shape[0]):
        begins = jnp.where(feature == doc, position, begins)
        position = position + lengths[doc]
        ends = jnp.where(feature == doc, position, ends)
    bounds[0:1] = begins.astype(jnp.float32)
    bounds[1:2] = ends.astype(jnp.float32)
    begins = jnp.broadcast_to(bounds[0:1], (HEAD_DIM, HEAD_DIM)).T
    ends = jnp.broadcast_to(bounds[1:2], (HEAD_DIM, HEAD_DIM)).T
    for tile in range(toks // HEAD_DIM):
        query_pos = (cp * toks + tile * HEAD_DIM + lax.broadcasted_iota(jnp.int32, (HEAD_DIM, HEAD_DIM), 1)).astype(jnp.float32)
        outside = (query_pos < begins) | (query_pos >= ends)
        outside = outside & (lax.broadcasted_iota(jnp.int32, (HEAD_DIM, HEAD_DIM), 0) <= lengths.shape[0])
        for k in range(PAIR):
            first = k * toks + tile * HEAD_DIM
            query_mask[:, first : first + HEAD_DIM] = jnp.where(outside, MASKED, 0.0).astype(jnp.bfloat16)

    def mark(side, block):
        key_pos = (block * toks + lax.broadcasted_iota(jnp.int32, (toks, HEAD_DIM), 0)).astype(jnp.float32)
        inside = (key_pos >= bounds[0:1]) & (key_pos < bounds[1:2])
        key_mask[side] = jnp.where(inside, 1.0, 0.0).astype(jnp.bfloat16)

    def product(keys, side, head, half, cut=slice(None)):
        return jnp.dot(
            jnp.concatenate([keys, key_mask[side]], axis=1),
            jnp.concatenate([qt[head, half, :, cut], query_mask[:, cut]], axis=0),
            preferred_element_type=jnp.float32)

    cuts = [slice(first, first + TILE) for first in range(0, PAIR * toks, TILE)]

    loads[4].wait()
    for h in range(heads):
        g, half, k = h // group, h % group // PAIR, h % PAIR
        qt[g, half, :, k * toks : (k + 1) * toks] = q_in[:, h * HEAD_DIM : (h + 1) * HEAD_DIM].T
    old_top[...] = jnp.zeros_like(old_top)
    new_top[...] = jnp.zeros_like(new_top)
    rescale[...] = jnp.ones_like(rescale)
    scores[1] = jnp.full(scores.shape[1:], MASKED, jnp.float32)
    weights[...] = jnp.zeros_like(weights)

    mark(1, cp)

    def own_body(head, carry):
        keys = kv[OWN, 0, head]
        values = kv[OWN, 1, head].T
        causal = lax.broadcasted_iota(jnp.int32, (toks, toks), 0) <= lax.broadcasted_iota(jnp.int32, (toks, toks), 1)
        for half in range(group // PAIR):
            found = product(keys, 1, head, half)
            found = jnp.concatenate(
                [jnp.where(causal, found[:, k * toks : (k + 1) * toks], MASKED) for k in range(PAIR)], axis=1)
            new = jnp.max(found, axis=0, keepdims=True)
            found = jnp.exp2((found - new) * factor)
            top[head, half] = new
            total[head, half] = jnp.sum(found, axis=0, keepdims=True)
            acc[head, half] = jnp.dot(values, found.astype(jnp.bfloat16), preferred_element_type=jnp.float32)
        return carry

    lax.fori_loop(0, kv_heads, own_body, 0)

    def where_is(step):
        in_pairs = jnp.where(core == 0, jnp.where(step < 8, step, step - 2), step - 2)
        far = jnp.where(core == 0, (step == 8) | (step == 9), step < 2)
        in_pairs = jnp.maximum(in_pairs, 0)
        distance = in_pairs // 4
        parity = lax.rem(in_pairs + step // 10, 2)
        slot = jnp.where(far, FAR, 2 * distance + parity)
        head = jnp.where(far, lax.rem(step, 2), lax.rem(in_pairs, 4) // 2)
        far_block = jnp.where(core == 0, 2 * chip - 7, 2 * chip)
        block = jnp.where(far, far_block, 2 * (chip - distance - 1) + parity)
        return slot, head, block

    def score(slot, head, half):
        keys, side = kv[slot, 0, head], lax.rem(slot, 2)
        for cut in cuts:
            found = product(keys, side, head, half, cut)
            scores[half, :, cut] = found
            old = top[head, half, :, cut]
            new = jnp.maximum(old, jnp.max(found, axis=0, keepdims=True))
            top[head, half, :, cut] = new
            old_top[half, :, cut] = old
            new_top[half, :, cut] = new

    def weigh(head, half):
        for cut in cuts:
            new = new_top[half, :, cut]
            shrink = jnp.exp2((old_top[half, :, cut] - new) * factor)
            found = jnp.exp2((scores[half, :, cut] - new) * factor)
            weights[half, :, cut] = found.astype(jnp.bfloat16)
            rescale[half, :, cut] = shrink
            total[head, half, :, cut] = total[head, half, :, cut] * shrink + jnp.sum(found, axis=0, keepdims=True)

    def gather(head, half, values):
        for cut in cuts:
            acc[head, half, :, cut] = acc[head, half, :, cut] * rescale[half, :, cut] + jnp.dot(
                values, weights[half, :, cut], preferred_element_type=jnp.float32)

    def finish(head):
        for h in range(group):
            half, cut = h // PAIR, slice(h % PAIR * toks, (h % PAIR + 1) * toks)
            first = (head * group + h) * HEAD_DIM
            share = 1.0 / total[head, half, :, cut]
            out[:, first : first + HEAD_DIM] = (acc[head, half, :, cut] * share).astype(out.dtype).T

    def step_body(step, carry):
        @pl.when(step == STEPS - 1)
        def _():
            finish(0)

        for quarter in range((STEPS + 3) // 4):
            @pl.when(step // 4 == quarter)
            def _():
                for s in range(4 * quarter, 4 * quarter + 4):
                    for me in (0, 1):
                        if s in AHEAD[me]:
                            @pl.when((step == s) & (core == me))
                            def _():
                                for slot, pieces in AHEAD[me][s]:
                                    event(me, slot, pieces)

        slot, head, block = where_is(step)
        last_slot, last_head, _ = where_is(jnp.maximum(step - 1, 0))

        @pl.when(head == 0)
        def _():
            mark(lax.rem(slot, 2), block)

        values = kv[last_slot, 1, last_head].T
        weigh(last_head, 1)
        score(slot, head, 0)
        gather(last_head, 0, values)
        score(slot, head, 1)
        gather(last_head, 1, values)
        weigh(head, 0)
        return carry

    lax.fori_loop(0, STEPS, step_body, 0)
    last_slot, last_head, _ = where_is(jnp.int32(STEPS - 1))
    values = kv[last_slot, 1, last_head].T
    weigh(last_head, 1)
    gather(last_head, 0, values)
    gather(last_head, 1, values)

    finish(kv_heads - 1)
    for me in (0, 1):
        @pl.when(core == me)
        def _():
            for p in range(4):
                for lane in OWN_LANES[me]:
                    if_known(own_send(lane, p), lambda copy: copy.wait_send())
                for slot in RELAYED[me]:
                    if relayed(me, slot, p):
                        if_known(relay(slot, p), lambda copy: copy.wait_send())
                for slot in CROSSED[me]:
                    if_known(cross(slot, p), lambda copy: copy.wait_send())


def body(count, queries, keys, values, lengths):
    toks, wide = queries.shape
    heads = wide // HEAD_DIM
    kv_heads = keys.shape[1] // HEAD_DIM
    group = heads // kv_heads
    return pl.pallas_call(
        functools.partial(kernel, count),
        out_shape=pltpu.VMEM((toks, wide), jnp.bfloat16),
        in_specs=[pl.BlockSpec(memory_space=pltpu.HBM)] * 3 + [pl.BlockSpec(memory_space=pltpu.SMEM)],
        out_specs=pl.BlockSpec(memory_space=pltpu.VMEM),
        scratch_shapes=[
            pltpu.VMEM((SLOTS, 2, kv_heads, toks, HEAD_DIM), jnp.bfloat16),
            pltpu.VMEM((toks, wide), jnp.bfloat16),
            pltpu.VMEM((kv_heads, group // PAIR, HEAD_DIM, PAIR * toks), jnp.bfloat16),
            pltpu.VMEM((kv_heads, group // PAIR, HEAD_DIM, PAIR * toks), jnp.float32),
            pltpu.VMEM((kv_heads, group // PAIR, 1, PAIR * toks), jnp.float32),
            pltpu.VMEM((kv_heads, group // PAIR, 1, PAIR * toks), jnp.float32),
            pltpu.VMEM((2, HEAD_DIM), jnp.float32),
            pltpu.VMEM((2, toks, HEAD_DIM), jnp.bfloat16),
            pltpu.VMEM((HEAD_DIM, PAIR * toks), jnp.bfloat16),
            pltpu.VMEM((2, toks, PAIR * toks), jnp.float32),
            pltpu.VMEM((2, toks, PAIR * toks), jnp.bfloat16),
            pltpu.VMEM((2, 1, PAIR * toks), jnp.float32),
            pltpu.VMEM((2, 1, PAIR * toks), jnp.float32),
            pltpu.VMEM((2, 1, PAIR * toks), jnp.float32),
            pltpu.SemaphoreType.DMA((5,)),
            pltpu.SemaphoreType.DMA((SLOTS, 4)),
            pltpu.SemaphoreType.DMA((4, 4)),
            pltpu.SemaphoreType.DMA((SLOTS, 4)),
            pltpu.SemaphoreType.DMA((SLOTS, 4)),
        ],
        compiler_params=pltpu.CompilerParams(collective_id=0, has_side_effects=True),
    )(queries, keys, values, lengths)


def solution(mesh):
    in_specs = (P("cp", "tp"), P("cp", "tp"), P("cp", "tp"), P())
    return jax.shard_map(functools.partial(body, mesh.shape["cp"]), mesh=mesh, in_specs=in_specs,
                         out_specs=P("cp", "tp"), check_vma=False)
```

```python
import functools
import math

import jax
import jax.numpy as jnp
from jax import lax
from jax.experimental import pallas as pl
from jax.experimental.pallas import tpu as pltpu
from jax.sharding import PartitionSpec as P

HEAD_DIM = 128
RING_Y = 8
PAIR = 2
MASKED = -1e30
TILE = 256
FAR = 6
LANDED = 7
RELAY = 8
OWN = 9
SPARE = 10
SLOTS = 11
FIRST, SECOND = (0, 1), (2, 3)
STEPS = 14
SHORT_WAY = (2, 3)
AHEAD = (
    {0: ((0, FIRST),), 1: ((1, FIRST),), 2: ((0, SECOND),), 3: ((1, SECOND),),
     4: ((2, FIRST),), 5: ((3, FIRST),), 6: ((2, SECOND),), 7: ((3, SECOND),),
     8: ((FAR, FIRST),), 9: ((FAR, SECOND),),
     10: ((4, (0,)), (5, FIRST)), 11: ((4, (1,)),), 12: ((5, SECOND), (4, (2,))), 13: ((4, (3,)),)},
    {0: ((FAR, FIRST),), 1: ((FAR, SECOND),),
     2: ((1, FIRST), (RELAY, (0,)), (SPARE, (0,)), (0, FIRST)),
     4: ((RELAY, (1,)), (SPARE, (1,)), (1, SECOND), (0, SECOND)),
     6: ((RELAY, (2,)), (SPARE, (2, 3)), (3, FIRST), (2, FIRST)),
     7: ((RELAY, (3,)), (LANDED, (0,))),
     8: ((LANDED, (1,)), (3, SECOND), (2, SECOND)), 9: ((LANDED, (2,)),),
     10: ((LANDED, (3,)), (5, (0,)), (5, (2,)), (5, (1,))), 11: ((5, (3,)), (4, FIRST)), 13: ((4, SECOND),)},
)
OWN_LANES = ((0, 1), (0, 2, 3))
RELAYED = ((0, 2), (1, 3, RELAY, LANDED, SPARE))
CROSSED = ((0, 2, 4), (1, 3, LANDED, 5))


def kernel(count, q_hbm, k_hbm, v_hbm, lengths, out,
           kv, q_in, qt, acc, top, total, bounds, key_mask, query_mask, scores, weights, old_top, new_top, rescale,
           load_sem, recv_sem, own_sem, relay_sem, cross_sem):
    toks = q_in.shape[0]
    kv_heads = kv.shape[2]
    heads = q_in.shape[1] // HEAD_DIM
    group = heads // kv_heads
    factor = HEAD_DIM ** -0.5 * math.log2(math.e)
    cp = lax.axis_index("cp")
    chip, core = cp // 2, lax.rem(cp, 2)
    chips = count // 2
    y = lax.rem(chip, RING_Y)
    row = chip - y

    def core_of(which_chip):
        return which_chip * 2 + core

    partner = chip * 2 + (1 - core)
    has_after, has_before = chip + 1 < chips, chip >= 1
    after, before = core_of(jnp.minimum(chip + 1, chips - 1)), core_of(jnp.maximum(chip - 1, 0))
    goes_down = chip + 4 < chips
    down = core_of(jnp.minimum(row + jnp.where(y >= 4, RING_Y, 0), chips - RING_Y) + lax.rem(y + RING_Y - 3, RING_Y))
    reader = row + lax.rem(y + RING_Y - 1, RING_Y)
    has_relay = reader >= 4
    relay_to, relay_owner = core_of(reader), core_of(jnp.maximum(reader - 4, 0))
    relay_from = core_of(row + lax.rem(y + 1, RING_Y))
    has_landed = chip >= 4
    owner_chip, reader_chip = chips - 4, chips - 1
    between_chip = owner_chip - owner_chip % RING_Y + (owner_chip + RING_Y - 3) % RING_Y
    is_owner, is_between, is_reader = chip == owner_chip, chip == between_chip, chip == reader_chip

    def holds(slot, me):
        if slot == RELAY:
            return has_relay
        if slot == SPARE:
            return is_between
        if slot == LANDED or (slot == FAR and me == 0):
            return has_landed
        if slot == FAR or slot == OWN:
            return chip >= 0
        return chip >= slot // 2 + 1

    def piece(slot, p):
        return kv.at[slot, p % 2, p // 2]

    def remote(src, dst, send, recv, to):
        return pltpu.make_async_remote_copy(
            src_ref=src, dst_ref=dst, send_sem=send, recv_sem=recv,
            device_id={"cp": to}, device_id_type=pl.DeviceIdType.MESH)

    loads = []
    for p in range(4):
        source = (k_hbm, v_hbm)[p % 2].at[:, pl.ds(p // 2 * HEAD_DIM, HEAD_DIM)]
        loads.append(pltpu.make_async_copy(source, piece(OWN, p), load_sem.at[p]))
    loads.append(pltpu.make_async_copy(q_hbm, q_in, load_sem.at[4]))
    for copy in loads:
        copy.start()

    barrier = pltpu.get_barrier_semaphore()

    def greet(peers):
        for known, device in peers:
            @pl.when(known)
            def _():
                pl.semaphore_signal(barrier, inc=1, device_id={"cp": device}, device_id_type=pl.DeviceIdType.MESH)
        pl.semaphore_wait(barrier, sum(known.astype(jnp.int32) for known, _ in peers))

    near = ((chip >= 0, partner), (has_after, after), (has_before, before))

    @pl.when(core == 0)
    def _():
        greet(near)

    @pl.when(core == 1)
    def _():
        greet(near + ((goes_down, down), (has_relay, relay_owner), (has_relay, relay_to), (has_landed, relay_from),
                      (is_owner | is_reader, core_of(between_chip)),
                      (is_between, core_of(owner_chip)), (is_between, core_of(reader_chip))))

    for copy in loads[:4]:
        copy.wait()

    def own_send(lane, p):
        to, slot = ((after, core), (partner, FAR), (down, RELAY), (core_of(between_chip), SPARE))[lane]
        return (has_after, chip >= 0, goes_down, is_owner)[lane], remote(
            piece(OWN, p), piece(slot, p), own_sem.at[lane, p], recv_sem.at[slot, p], to)

    def relay(slot, p):
        to, target = {0: (after, 2), 1: (after, 3), 2: (after, 4), 3: (after, 5),
                      RELAY: (relay_to, LANDED), LANDED: (before, 5), SPARE: (core_of(reader_chip), 5)}[slot]
        known = holds(slot, 1)
        if slot < FAR:
            known = known & has_after
        return known, remote(piece(slot, p), piece(target, p), relay_sem.at[slot, p], recv_sem.at[target, p], to)

    def relayed(me, slot, p):
        if slot == 3 and p not in SHORT_WAY or slot in (LANDED, SPARE) and p in SHORT_WAY:
            return False
        return slot in RELAYED[me]

    def cross(slot, p):
        target = FAR if slot == LANDED else slot
        return holds(slot, 1), remote(piece(slot, p), piece(target, p), cross_sem.at[slot, p], recv_sem.at[target, p], partner)

    def if_known(known_and_copy, act):
        known, copy = known_and_copy

        @pl.when(known)
        def _():
            act(copy)

    def event(me, slot, pieces):
        for p in pieces:
            @pl.when(holds(slot, me))
            def _():
                remote(piece(slot, p), piece(slot, p), cross_sem.at[slot, p], recv_sem.at[slot, p], partner).wait_recv()
                if relayed(me, slot, p):
                    if_known(relay(slot, p), lambda copy: copy.start())
                if slot in CROSSED[me]:
                    cross(slot, p)[1].start()

    for me in (0, 1):
        @pl.when(core == me)
        def _():
            for p in range(4):
                for lane in OWN_LANES[me]:
                    if_known(own_send(lane, p), lambda copy: copy.start())

    for slot in range(FAR + 1):
        @pl.when(~(holds(slot, 1) if slot < FAR else (holds(FAR, 0) | (core == 1))))
        def _():
            kv[slot] = jnp.zeros(kv.shape[1:], kv.dtype)

    feature = lax.broadcasted_iota(jnp.int32, (1, HEAD_DIM), 1)
    begins = jnp.where(feature == lengths.shape[0], -(1 << 20), jnp.full((1, HEAD_DIM), 1 << 20, jnp.int32))
    ends = jnp.zeros((1, HEAD_DIM), jnp.int32)
    position = jnp.int32(0)
    for doc in range(lengths.shape[0]):
        begins = jnp.where(feature == doc, position, begins)
        position = position + lengths[doc]
        ends = jnp.where(feature == doc, position, ends)
    bounds[0:1] = begins.astype(jnp.float32)
    bounds[1:2] = ends.astype(jnp.float32)
    begins = jnp.broadcast_to(bounds[0:1], (HEAD_DIM, HEAD_DIM)).T
    ends = jnp.broadcast_to(bounds[1:2], (HEAD_DIM, HEAD_DIM)).T
    for tile in range(toks // HEAD_DIM):
        query_pos = (cp * toks + tile * HEAD_DIM + lax.broadcasted_iota(jnp.int32, (HEAD_DIM, HEAD_DIM), 1)).astype(jnp.float32)
        outside = (query_pos < begins) | (query_pos >= ends)
        outside = outside & (lax.broadcasted_iota(jnp.int32, (HEAD_DIM, HEAD_DIM), 0) <= lengths.shape[0])
        for k in range(PAIR):
            first = k * toks + tile * HEAD_DIM
            query_mask[:, first : first + HEAD_DIM] = jnp.where(outside, MASKED, 0.0).astype(jnp.bfloat16)

    def mark(side, block):
        key_pos = (block * toks + lax.broadcasted_iota(jnp.int32, (toks, HEAD_DIM), 0)).astype(jnp.float32)
        inside = (key_pos >= bounds[0:1]) & (key_pos < bounds[1:2])
        key_mask[side] = jnp.where(inside, 1.0, 0.0).astype(jnp.bfloat16)

    def product(keys, side, head, half, cut=slice(None)):
        return jnp.dot(
            jnp.concatenate([keys, key_mask[side]], axis=1),
            jnp.concatenate([qt[head, half, :, cut], query_mask[:, cut]], axis=0),
            preferred_element_type=jnp.float32)

    cuts = [slice(first, first + TILE) for first in range(0, PAIR * toks, TILE)]

    loads[4].wait()
    for h in range(heads):
        g, half, k = h // group, h % group // PAIR, h % PAIR
        qt[g, half, :, k * toks : (k + 1) * toks] = q_in[:, h * HEAD_DIM : (h + 1) * HEAD_DIM].T
    old_top[...] = jnp.zeros_like(old_top)
    new_top[...] = jnp.zeros_like(new_top)
    rescale[...] = jnp.ones_like(rescale)
    scores[1] = jnp.full(scores.shape[1:], MASKED, jnp.float32)
    weights[...] = jnp.zeros_like(weights)

    mark(OWN, cp)

    def own_body(head, carry):
        keys = kv[OWN, 0, head]
        values = kv[OWN, 1, head].T
        causal = lax.broadcasted_iota(jnp.int32, (toks, toks), 0) <= lax.broadcasted_iota(jnp.int32, (toks, toks), 1)
        for half in range(group // PAIR):
            found = product(keys, OWN, head, half)
            found = jnp.concatenate(
                [jnp.where(causal, found[:, k * toks : (k + 1) * toks], MASKED) for k in range(PAIR)], axis=1)
            new = jnp.max(found, axis=0, keepdims=True)
            found = jnp.exp2((found - new) * factor)
            top[head, half] = new
            total[head, half] = jnp.sum(found, axis=0, keepdims=True)
            acc[head, half] = jnp.dot(values, found.astype(jnp.bfloat16), preferred_element_type=jnp.float32)
        return carry

    lax.fori_loop(0, kv_heads, own_body, 0)

    def mark_body(slot, carry):
        far_block = jnp.where(core == 0, 2 * chip - 7, 2 * chip)
        mark(slot, jnp.where(slot == FAR, far_block, 2 * (chip - slot // 2 - 1) + lax.rem(slot, 2)))
        return carry

    lax.fori_loop(0, FAR + 1, mark_body, 0)

    def where_is(step):
        in_pairs = jnp.where(core == 0, jnp.where(step < 8, step, step - 2), step - 2)
        far = jnp.where(core == 0, (step == 8) | (step == 9), step < 2)
        in_pairs = jnp.maximum(in_pairs, 0)
        distance = in_pairs // 4
        parity = lax.rem(in_pairs + step // 10, 2)
        slot = jnp.where(far, FAR, 2 * distance + parity)
        head = jnp.where(far, lax.rem(step, 2), lax.rem(in_pairs, 4) // 2)
        return slot, head

    def score(slot, head, half):
        keys, side = kv[slot, 0, head], slot
        for cut in cuts:
            found = product(keys, side, head, half, cut)
            scores[half, :, cut] = found
            old = top[head, half, :, cut]
            new = jnp.maximum(old, jnp.max(found, axis=0, keepdims=True))
            top[head, half, :, cut] = new
            old_top[half, :, cut] = old
            new_top[half, :, cut] = new

    def weigh(head, half):
        for cut in cuts:
            new = new_top[half, :, cut]
            shrink = jnp.exp2((old_top[half, :, cut] - new) * factor)
            found = jnp.exp2((scores[half, :, cut] - new) * factor)
            weights[half, :, cut] = found.astype(jnp.bfloat16)
            rescale[half, :, cut] = shrink
            total[head, half, :, cut] = total[head, half, :, cut] * shrink + jnp.sum(found, axis=0, keepdims=True)

    def gather(head, half, values):
        for cut in cuts:
            acc[head, half, :, cut] = acc[head, half, :, cut] * rescale[half, :, cut] + jnp.dot(
                values, weights[half, :, cut], preferred_element_type=jnp.float32)

    def finish(head):
        for h in range(group):
            half, cut = h // PAIR, slice(h % PAIR * toks, (h % PAIR + 1) * toks)
            first = (head * group + h) * HEAD_DIM
            share = 1.0 / total[head, half, :, cut]
            out[:, first : first + HEAD_DIM] = (acc[head, half, :, cut] * share).astype(out.dtype).T

    def step_body(step, carry):
        for quarter in range((STEPS + 3) // 4):
            @pl.when(step // 4 == quarter)
            def _():
                for s in range(4 * quarter, min(4 * quarter + 4, STEPS - 1)):
                    for me in (0, 1):
                        if s in AHEAD[me]:
                            @pl.when((step == s) & (core == me))
                            def _():
                                for slot, pieces in AHEAD[me][s]:
                                    event(me, slot, pieces)

        slot, head = where_is(step)
        last_slot, last_head = where_is(jnp.maximum(step - 1, 0))

        values = kv[last_slot, 1, last_head].T
        weigh(last_head, 1)
        score(slot, head, 0)
        gather(last_head, 0, values)
        score(slot, head, 1)
        gather(last_head, 1, values)
        weigh(head, 0)
        return carry

    lax.fori_loop(0, STEPS - 1, step_body, 0)
    last_slot, last_head = where_is(jnp.int32(STEPS - 2))
    values = kv[last_slot, 1, last_head].T
    weigh(last_head, 1)
    gather(last_head, 0, values)
    gather(last_head, 1, values)
    for head in range(kv_heads - 1):
        finish(head)
    for me in (0, 1):
        @pl.when(core == me)
        def _():
            for slot, pieces in AHEAD[me][STEPS - 1]:
                event(me, slot, pieces)

    head = kv_heads - 1
    values = kv[4, 1, head].T
    score(4, head, 0)
    score(4, head, 1)
    for half in range(group // PAIR):
        weigh(head, half)
        gather(head, half, values)
    finish(head)
    for me in (0, 1):
        @pl.when(core == me)
        def _():
            for p in range(4):
                for lane in OWN_LANES[me]:
                    if_known(own_send(lane, p), lambda copy: copy.wait_send())
                for slot in RELAYED[me]:
                    if relayed(me, slot, p):
                        if_known(relay(slot, p), lambda copy: copy.wait_send())
                for slot in CROSSED[me]:
                    if_known(cross(slot, p), lambda copy: copy.wait_send())


def body(count, queries, keys, values, lengths):
    toks, wide = queries.shape
    heads = wide // HEAD_DIM
    kv_heads = keys.shape[1] // HEAD_DIM
    group = heads // kv_heads
    return pl.pallas_call(
        functools.partial(kernel, count),
        out_shape=pltpu.VMEM((toks, wide), jnp.bfloat16),
        in_specs=[pl.BlockSpec(memory_space=pltpu.HBM)] * 3 + [pl.BlockSpec(memory_space=pltpu.SMEM)],
        out_specs=pl.BlockSpec(memory_space=pltpu.VMEM),
        scratch_shapes=[
            pltpu.VMEM((SLOTS, 2, kv_heads, toks, HEAD_DIM), jnp.bfloat16),
            pltpu.VMEM((toks, wide), jnp.bfloat16),
            pltpu.VMEM((kv_heads, group // PAIR, HEAD_DIM, PAIR * toks), jnp.bfloat16),
            pltpu.VMEM((kv_heads, group // PAIR, HEAD_DIM, PAIR * toks), jnp.float32),
            pltpu.VMEM((kv_heads, group // PAIR, 1, PAIR * toks), jnp.float32),
            pltpu.VMEM((kv_heads, group // PAIR, 1, PAIR * toks), jnp.float32),
            pltpu.VMEM((2, HEAD_DIM), jnp.float32),
            pltpu.VMEM((SLOTS, toks, HEAD_DIM), jnp.bfloat16),
            pltpu.VMEM((HEAD_DIM, PAIR * toks), jnp.bfloat16),
            pltpu.VMEM((2, toks, PAIR * toks), jnp.float32),
            pltpu.VMEM((2, toks, PAIR * toks), jnp.bfloat16),
            pltpu.VMEM((2, 1, PAIR * toks), jnp.float32),
            pltpu.VMEM((2, 1, PAIR * toks), jnp.float32),
            pltpu.VMEM((2, 1, PAIR * toks), jnp.float32),
            pltpu.SemaphoreType.DMA((5,)),
            pltpu.SemaphoreType.DMA((SLOTS, 4)),
            pltpu.SemaphoreType.DMA((4, 4)),
            pltpu.SemaphoreType.DMA((SLOTS, 4)),
            pltpu.SemaphoreType.DMA((SLOTS, 4)),
        ],
        compiler_params=pltpu.CompilerParams(collective_id=0, has_side_effects=True),
    )(queries, keys, values, lengths)


def solution(mesh):
    in_specs = (P("cp", "tp"), P("cp", "tp"), P("cp", "tp"), P())
    return jax.shard_map(functools.partial(body, mesh.shape["cp"]), mesh=mesh, in_specs=in_specs,
                         out_specs=P("cp", "tp"), check_vma=False)
```

```python
import functools
import math

import jax
import jax.numpy as jnp
from jax import lax
from jax.experimental import pallas as pl
from jax.experimental.pallas import tpu as pltpu
from jax.sharding import PartitionSpec as P

HEAD_DIM = 128
RING_Y = 8
PAIR = 2
MASKED = -1e30
TILE = 256
FAR = 6
LANDED = 7
RELAY = 8
OWN = 9
SLOTS = 10
FIRST, SECOND = (0, 1), (2, 3)
STEPS = 14
SHORT_WAY = (3,)
AHEAD = (
    {0: ((0, FIRST),), 1: ((1, FIRST),), 2: ((0, SECOND),), 3: ((1, SECOND),),
     4: ((2, FIRST),), 5: ((3, FIRST),), 6: ((2, SECOND),), 7: ((3, SECOND),),
     8: ((FAR, FIRST),), 9: ((FAR, SECOND),),
     10: ((4, (0,)), (5, FIRST)), 11: ((4, (1,)),), 12: ((5, SECOND), (4, (2,))), 13: ((4, (3,)),)},
    {0: ((FAR, FIRST),), 1: ((FAR, SECOND),),
     2: ((1, FIRST), (RELAY, (0,)), (0, FIRST)),
     4: ((RELAY, (1,)), (1, SECOND), (0, SECOND)),
     6: ((RELAY, (2,)), (3, FIRST), (2, FIRST)),
     7: ((RELAY, (3,)), (LANDED, (0,))),
     8: ((LANDED, (1,)), (3, SECOND), (2, SECOND)), 9: ((LANDED, (2,)),),
     10: ((LANDED, (3,)), (5, (0, 1))), 11: ((5, SECOND), (4, FIRST)), 13: ((4, SECOND),)},
)
OWN_LANES = ((0, 1), (2, 0))
RELAYED = ((0, 2), (1, 3, RELAY, LANDED))
CROSSED = ((0, 2, 4), (1, 3, LANDED, 5))


def kernel(count, q_hbm, k_hbm, v_hbm, lengths, out,
           kv, q_in, qt, acc, top, total, bounds, key_mask, query_mask, scores, weights, old_top, new_top, rescale,
           load_sem, recv_sem, own_sem, relay_sem, cross_sem):
    toks = q_in.shape[0]
    kv_heads = kv.shape[2]
    heads = q_in.shape[1] // HEAD_DIM
    group = heads // kv_heads
    factor = HEAD_DIM ** -0.5 * math.log2(math.e)
    cp = lax.axis_index("cp")
    chip, core = cp // 2, lax.rem(cp, 2)
    chips = count // 2
    y = lax.rem(chip, RING_Y)
    row = chip - y

    def core_of(which_chip):
        return which_chip * 2 + core

    partner = chip * 2 + (1 - core)
    has_after, has_before = chip + 1 < chips, chip >= 1
    after, before = core_of(jnp.minimum(chip + 1, chips - 1)), core_of(jnp.maximum(chip - 1, 0))
    goes_down = chip + 4 < chips
    down = core_of(jnp.minimum(row + jnp.where(y >= 4, RING_Y, 0), chips - RING_Y) + lax.rem(y + RING_Y - 3, RING_Y))
    reader = row + lax.rem(y + RING_Y - 1, RING_Y)
    has_relay = reader >= 4
    relay_to, relay_owner = core_of(reader), core_of(jnp.maximum(reader - 4, 0))
    relay_from = core_of(row + lax.rem(y + 1, RING_Y))
    has_landed = chip >= 4

    def holds(slot, me):
        if slot == RELAY:
            return has_relay
        if slot == LANDED or (slot == FAR and me == 0):
            return has_landed
        if slot == FAR or slot == OWN:
            return chip >= 0
        return chip >= slot // 2 + 1

    def piece(slot, p):
        return kv.at[slot, p % 2, p // 2]

    def remote(src, dst, send, recv, to):
        return pltpu.make_async_remote_copy(
            src_ref=src, dst_ref=dst, send_sem=send, recv_sem=recv,
            device_id={"cp": to}, device_id_type=pl.DeviceIdType.MESH)

    loads = []
    for p in range(4):
        source = (k_hbm, v_hbm)[p % 2].at[:, pl.ds(p // 2 * HEAD_DIM, HEAD_DIM)]
        loads.append(pltpu.make_async_copy(source, piece(OWN, p), load_sem.at[p]))
    loads.append(pltpu.make_async_copy(q_hbm, q_in, load_sem.at[4]))
    for copy in loads:
        copy.start()

    barrier = pltpu.get_barrier_semaphore()

    def greet(peers):
        for known, device in peers:
            @pl.when(known)
            def _():
                pl.semaphore_signal(barrier, inc=1, device_id={"cp": device}, device_id_type=pl.DeviceIdType.MESH)
        pl.semaphore_wait(barrier, sum(known.astype(jnp.int32) for known, _ in peers))

    near = ((chip >= 0, partner), (has_after, after), (has_before, before))

    @pl.when(core == 0)
    def _():
        greet(near)

    @pl.when(core == 1)
    def _():
        greet(near + ((goes_down, down), (has_relay, relay_owner), (has_relay, relay_to), (has_landed, relay_from)))

    for copy in loads[:4]:
        copy.wait()

    def own_send(lane, p):
        to, slot = ((after, core), (partner, FAR), (down, RELAY))[lane]
        return (has_after, chip >= 0, goes_down)[lane], remote(
            piece(OWN, p), piece(slot, p), own_sem.at[lane, p], recv_sem.at[slot, p], to)

    def relay(slot, p):
        to, target = {0: (after, 2), 1: (after, 3), 2: (after, 4), 3: (after, 5),
                      RELAY: (relay_to, LANDED), LANDED: (before, 5)}[slot]
        known = holds(slot, 1)
        if slot < FAR:
            known = known & has_after
        if slot == 3 and p not in SHORT_WAY:
            known = known & (y == RING_Y - 2)
        if slot == LANDED:
            known = known & (y != 0)
        return known, remote(piece(slot, p), piece(target, p), relay_sem.at[slot, p], recv_sem.at[target, p], to)

    def relayed(me, slot, p):
        if slot == LANDED and p in SHORT_WAY:
            return False
        return slot in RELAYED[me]

    def cross(slot, p):
        target = FAR if slot == LANDED else slot
        return holds(slot, 1), remote(piece(slot, p), piece(target, p), cross_sem.at[slot, p], recv_sem.at[target, p], partner)

    def if_known(known_and_copy, act):
        known, copy = known_and_copy

        @pl.when(known)
        def _():
            act(copy)

    def event(me, slot, pieces):
        for p in pieces:
            @pl.when(holds(slot, me))
            def _():
                remote(piece(slot, p), piece(slot, p), cross_sem.at[slot, p], recv_sem.at[slot, p], partner).wait_recv()
                if relayed(me, slot, p):
                    if_known(relay(slot, p), lambda copy: copy.start())
                if slot in CROSSED[me]:
                    cross(slot, p)[1].start()

    for me in (0, 1):
        @pl.when(core == me)
        def _():
            for p in range(4):
                for lane in OWN_LANES[me]:
                    if_known(own_send(lane, p), lambda copy: copy.start())

    for slot in range(FAR + 1):
        @pl.when(~(holds(slot, 1) if slot < FAR else (holds(FAR, 0) | (core == 1))))
        def _():
            kv[slot] = jnp.zeros(kv.shape[1:], kv.dtype)

    feature = lax.broadcasted_iota(jnp.int32, (1, HEAD_DIM), 1)
    begins = jnp.where(feature == lengths.shape[0], -(1 << 20), jnp.full((1, HEAD_DIM), 1 << 20, jnp.int32))
    ends = jnp.zeros((1, HEAD_DIM), jnp.int32)
    position = jnp.int32(0)
    for doc in range(lengths.shape[0]):
        begins = jnp.where(feature == doc, position, begins)
        position = position + lengths[doc]
        ends = jnp.where(feature == doc, position, ends)
    bounds[0:1] = begins.astype(jnp.float32)
    bounds[1:2] = ends.astype(jnp.float32)
    begins = jnp.broadcast_to(bounds[0:1], (HEAD_DIM, HEAD_DIM)).T
    ends = jnp.broadcast_to(bounds[1:2], (HEAD_DIM, HEAD_DIM)).T
    for tile in range(toks // HEAD_DIM):
        query_pos = (cp * toks + tile * HEAD_DIM + lax.broadcasted_iota(jnp.int32, (HEAD_DIM, HEAD_DIM), 1)).astype(jnp.float32)
        outside = (query_pos < begins) | (query_pos >= ends)
        outside = outside & (lax.broadcasted_iota(jnp.int32, (HEAD_DIM, HEAD_DIM), 0) <= lengths.shape[0])
        for k in range(PAIR):
            first = k * toks + tile * HEAD_DIM
            query_mask[:, first : first + HEAD_DIM] = jnp.where(outside, MASKED, 0.0).astype(jnp.bfloat16)

    def mark(side, block):
        key_pos = (block * toks + lax.broadcasted_iota(jnp.int32, (toks, HEAD_DIM), 0)).astype(jnp.float32)
        inside = (key_pos >= bounds[0:1]) & (key_pos < bounds[1:2])
        key_mask[side] = jnp.where(inside, 1.0, 0.0).astype(jnp.bfloat16)

    def product(keys, side, head, half, cut=slice(None)):
        return jnp.dot(
            jnp.concatenate([keys, key_mask[side]], axis=1),
            jnp.concatenate([qt[head, half, :, cut], query_mask[:, cut]], axis=0),
            preferred_element_type=jnp.float32)

    cuts = [slice(first, first + TILE) for first in range(0, PAIR * toks, TILE)]

    loads[4].wait()
    for h in range(heads):
        g, half, k = h // group, h % group // PAIR, h % PAIR
        qt[g, half, :, k * toks : (k + 1) * toks] = q_in[:, h * HEAD_DIM : (h + 1) * HEAD_DIM].T
    old_top[...] = jnp.zeros_like(old_top)
    new_top[...] = jnp.zeros_like(new_top)
    rescale[...] = jnp.ones_like(rescale)
    scores[1] = jnp.full(scores.shape[1:], MASKED, jnp.float32)
    weights[...] = jnp.zeros_like(weights)

    mark(OWN, cp)

    def own_body(head, carry):
        keys = kv[OWN, 0, head]
        values = kv[OWN, 1, head].T
        causal = lax.broadcasted_iota(jnp.int32, (toks, toks), 0) <= lax.broadcasted_iota(jnp.int32, (toks, toks), 1)
        for half in range(group // PAIR):
            found = product(keys, OWN, head, half)
            found = jnp.concatenate(
                [jnp.where(causal, found[:, k * toks : (k + 1) * toks], MASKED) for k in range(PAIR)], axis=1)
            new = jnp.max(found, axis=0, keepdims=True)
            found = jnp.exp2((found - new) * factor)
            top[head, half] = new
            total[head, half] = jnp.sum(found, axis=0, keepdims=True)
            acc[head, half] = jnp.dot(values, found.astype(jnp.bfloat16), preferred_element_type=jnp.float32)
        return carry

    lax.fori_loop(0, kv_heads, own_body, 0)

    def mark_body(slot, carry):
        far_block = jnp.where(core == 0, 2 * chip - 7, 2 * chip)
        mark(slot, jnp.where(slot == FAR, far_block, 2 * (chip - slot // 2 - 1) + lax.rem(slot, 2)))
        return carry

    lax.fori_loop(0, FAR + 1, mark_body, 0)

    def where_is(step):
        in_pairs = jnp.where(core == 0, jnp.where(step < 8, step, step - 2), step - 2)
        far = jnp.where(core == 0, (step == 8) | (step == 9), step < 2)
        in_pairs = jnp.maximum(in_pairs, 0)
        distance = in_pairs // 4
        parity = lax.rem(in_pairs + step // 10, 2)
        slot = jnp.where(far, FAR, 2 * distance + parity)
        head = jnp.where(far, lax.rem(step, 2), lax.rem(in_pairs, 4) // 2)
        return slot, head

    def score(slot, head, half):
        keys, side = kv[slot, 0, head], slot
        for cut in cuts:
            found = product(keys, side, head, half, cut)
            scores[half, :, cut] = found
            old = top[head, half, :, cut]
            new = jnp.maximum(old, jnp.max(found, axis=0, keepdims=True))
            top[head, half, :, cut] = new
            old_top[half, :, cut] = old
            new_top[half, :, cut] = new

    def weigh(head, half):
        for cut in cuts:
            new = new_top[half, :, cut]
            shrink = jnp.exp2((old_top[half, :, cut] - new) * factor)
            found = jnp.exp2((scores[half, :, cut] - new) * factor)
            weights[half, :, cut] = found.astype(jnp.bfloat16)
            rescale[half, :, cut] = shrink
            total[head, half, :, cut] = total[head, half, :, cut] * shrink + jnp.sum(found, axis=0, keepdims=True)

    def gather(head, half, values):
        for cut in cuts:
            acc[head, half, :, cut] = acc[head, half, :, cut] * rescale[half, :, cut] + jnp.dot(
                values, weights[half, :, cut], preferred_element_type=jnp.float32)

    def finish(head):
        for h in range(group):
            half, cut = h // PAIR, slice(h % PAIR * toks, (h % PAIR + 1) * toks)
            first = (head * group + h) * HEAD_DIM
            share = 1.0 / total[head, half, :, cut]
            out[:, first : first + HEAD_DIM] = (acc[head, half, :, cut] * share).astype(out.dtype).T

    def step_body(step, carry):
        for quarter in range((STEPS + 3) // 4):
            @pl.when(step // 4 == quarter)
            def _():
                for s in range(4 * quarter, min(4 * quarter + 4, STEPS - 1)):
                    for me in (0, 1):
                        if s in AHEAD[me]:
                            @pl.when((step == s) & (core == me))
                            def _():
                                for slot, pieces in AHEAD[me][s]:
                                    event(me, slot, pieces)

        slot, head = where_is(step)
        last_slot, last_head = where_is(jnp.maximum(step - 1, 0))

        values = kv[last_slot, 1, last_head].T
        weigh(last_head, 1)
        score(slot, head, 0)
        gather(last_head, 0, values)
        score(slot, head, 1)
        gather(last_head, 1, values)
        weigh(head, 0)
        return carry

    lax.fori_loop(0, STEPS - 1, step_body, 0)
    last_slot, last_head = where_is(jnp.int32(STEPS - 2))
    values = kv[last_slot, 1, last_head].T
    weigh(last_head, 1)
    gather(last_head, 0, values)
    gather(last_head, 1, values)
    for head in range(kv_heads - 1):
        finish(head)
    for me in (0, 1):
        @pl.when(core == me)
        def _():
            for slot, pieces in AHEAD[me][STEPS - 1]:
                event(me, slot, pieces)

    head = kv_heads - 1
    values = kv[4, 1, head].T
    score(4, head, 0)
    score(4, head, 1)
    for half in range(group // PAIR):
        weigh(head, half)
        gather(head, half, values)
    finish(head)
    for me in (0, 1):
        @pl.when(core == me)
        def _():
            for p in range(4):
                for lane in OWN_LANES[me]:
                    if_known(own_send(lane, p), lambda copy: copy.wait_send())
                for slot in RELAYED[me]:
                    if relayed(me, slot, p):
                        if_known(relay(slot, p), lambda copy: copy.wait_send())
                for slot in CROSSED[me]:
                    if_known(cross(slot, p), lambda copy: copy.wait_send())


def body(count, queries, keys, values, lengths):
    toks, wide = queries.shape
    heads = wide // HEAD_DIM
    kv_heads = keys.shape[1] // HEAD_DIM
    group = heads // kv_heads
    return pl.pallas_call(
        functools.partial(kernel, count),
        out_shape=pltpu.VMEM((toks, wide), jnp.bfloat16),
        in_specs=[pl.BlockSpec(memory_space=pltpu.HBM)] * 3 + [pl.BlockSpec(memory_space=pltpu.SMEM)],
        out_specs=pl.BlockSpec(memory_space=pltpu.VMEM),
        scratch_shapes=[
            pltpu.VMEM((SLOTS, 2, kv_heads, toks, HEAD_DIM), jnp.bfloat16),
            pltpu.VMEM((toks, wide), jnp.bfloat16),
            pltpu.VMEM((kv_heads, group // PAIR, HEAD_DIM, PAIR * toks), jnp.bfloat16),
            pltpu.VMEM((kv_heads, group // PAIR, HEAD_DIM, PAIR * toks), jnp.float32),
            pltpu.VMEM((kv_heads, group // PAIR, 1, PAIR * toks), jnp.float32),
            pltpu.VMEM((kv_heads, group // PAIR, 1, PAIR * toks), jnp.float32),
            pltpu.VMEM((2, HEAD_DIM), jnp.float32),
            pltpu.VMEM((SLOTS, toks, HEAD_DIM), jnp.bfloat16),
            pltpu.VMEM((HEAD_DIM, PAIR * toks), jnp.bfloat16),
            pltpu.VMEM((2, toks, PAIR * toks), jnp.float32),
            pltpu.VMEM((2, toks, PAIR * toks), jnp.bfloat16),
            pltpu.VMEM((2, 1, PAIR * toks), jnp.float32),
            pltpu.VMEM((2, 1, PAIR * toks), jnp.float32),
            pltpu.VMEM((2, 1, PAIR * toks), jnp.float32),
            pltpu.SemaphoreType.DMA((5,)),
            pltpu.SemaphoreType.DMA((SLOTS, 4)),
            pltpu.SemaphoreType.DMA((3, 4)),
            pltpu.SemaphoreType.DMA((SLOTS, 4)),
            pltpu.SemaphoreType.DMA((SLOTS, 4)),
        ],
        compiler_params=pltpu.CompilerParams(collective_id=0, has_side_effects=True),
    )(queries, keys, values, lengths)


def solution(mesh):
    in_specs = (P("cp", "tp"), P("cp", "tp"), P("cp", "tp"), P())
    return jax.shard_map(functools.partial(body, mesh.shape["cp"]), mesh=mesh, in_specs=in_specs,
                         out_specs=P("cp", "tp"), check_vma=False)
```
